32 devices in a mesh: seq: 4 (over y, x), exp: 8 (over z, core).
Axes of the slice: x: 2, y: 2, z: 4, core: 2. Of those that a mesh axis runs over, the one named last changes fastest.
Arguments:
- tokens: bfloat16 [2, 24576, 1024], P(None, ('seq', 'exp')), may hold values from -60 to 60
- router: bfloat16 [1024, 64], replicated, may hold values from -0.25 to 0.25
- w_in: bfloat16 [16, 1024, 4096], P('exp', None, 'seq'), may hold values from -0.1875 to 0.1875
- w_out: bfloat16 [16, 4096, 1024], P('exp', 'seq'), may hold values from -0.09375 to 0.09375
- grad_out: bfloat16 [2, 24576, 1024], P(None, ('seq', 'exp')), may hold values from -6 to 6
Outputs:
- mixed: bfloat16 [2, 24576, 1024], P(None, ('seq', 'exp'))
- grad_tokens: bfloat16 [2, 24576, 1024], P(None, ('seq', 'exp'))
- grad_router: float32 [1024, 64], P(('seq', 'exp'))
- grad_w_in: bfloat16 [16, 1024, 4096], P('exp', None, 'seq')
- grad_w_out: bfloat16 [16, 4096, 1024], P('exp', 'seq')
The draws below stay inside these ranges and needn't reach their ends.
All inputs are finite; a program needn't handle non-finite values.
Results may differ from the reference program's by a relative error of at most 0.018.
Values may be sent and summed in bfloat16 or wider, within the bound.
A program may use at most 128 MiB of HBM per device.

```python
import math
import jax
import jax.numpy as jnp
from jax import lax

D = 1024
FF = 4096
SLOTS = 4
CLIPS = 2
EXPERTS = 16
SLOT_COUNT = 64
TOKENS = 24576


def router_base(key):
    base = jax.random.normal(jax.random.fold_in(key, 7), (D, SLOT_COUNT), jnp.float32) / math.sqrt(D)
    return jnp.clip(base, -0.25, 0.25)


def draw_router(key, part):
    return router_base(key).astype(jnp.bfloat16)


def draw_tokens(key, part):
    values = jax.random.normal(jax.random.fold_in(key, 11), (CLIPS, TOKENS, D), jnp.float32)
    return jnp.clip(values, -6.0, 6.0).astype(jnp.bfloat16)


def block_levels(key, shape, split, least, top_value):
    def one(dim, blocks):
        steps = jax.random.uniform(jax.random.fold_in(jax.random.fold_in(key, 6), dim), (blocks,), jnp.float32, least / len(split), top_value / len(split))
        return jnp.repeat(jnp.exp(steps), shape[dim] // blocks).reshape((-1,) + (1,) * (len(shape) - dim - 1))

    loudness = one(*split[0])
    for cut in split[1:]:
        loudness = loudness * one(*cut)
    return loudness


def gaussian(stream_key, dims, spread, limit, split=(), kind=jnp.bfloat16):
    gain = block_levels(stream_key, dims, split, -0.22, 0.18) if split else 1.0
    array = jax.random.normal(stream_key, dims, jnp.float32) * spread * gain
    return jnp.minimum(jnp.maximum(array, -limit), limit).astype(kind)


def setup_inputs(seed: int = 0) -> dict:
    keys = jax.random.split(jax.random.key(seed), 6)
    return {
        "tokens": draw_tokens(jax.random.fold_in(keys[5], 71), 0),
        "router": draw_router(jax.random.fold_in(keys[5], 71), 0),
        "w_in": gaussian(keys[2], (EXPERTS, D, FF), D ** -0.5, 0.1875, ((0, 8), (2, 4))),
        "w_out": gaussian(keys[3], (EXPERTS, FF, D), FF ** -0.5, 0.09375, ((0, 8), (1, 4))),
        "grad_out": gaussian(keys[4], (CLIPS, TOKENS, D), 1.0, 6.0, ((1, 32),)),
    }


def reference(tokens, router, w_in, w_out, grad_out):
    width = tokens.shape[2]
    slot_total = router.shape[1]
    experts = w_in.shape[0]
    tokens_f = tokens.astype(jnp.float32)
    grad_f = grad_out.astype(jnp.float32)
    logits = jnp.dot(tokens.reshape(CLIPS * TOKENS, width).astype(jnp.float32), router.astype(jnp.float32), preferred_element_type=jnp.float32).reshape(CLIPS, TOKENS, slot_total)
    slot_peak = lax.optimization_barrier(jnp.max(logits, axis=1, keepdims=True))
    exp_terms = jnp.exp(logits - slot_peak)
    dispatch = exp_terms / lax.optimization_barrier(jnp.sum(exp_terms, axis=1, keepdims=True))
    dispatch_b = dispatch.astype(jnp.bfloat16)
    mixing = jax.nn.softmax(logits, axis=2)
    mixing_b = mixing.astype(jnp.bfloat16)
    slot_in = jnp.einsum('cts,ctd->scd', dispatch_b.astype(jnp.float32), tokens_f).astype(jnp.bfloat16)
    expert_rows = slot_in.reshape(experts, SLOTS * CLIPS, width)
    pre = jnp.einsum('erd,edh->erh', expert_rows.astype(jnp.float32), w_in.astype(jnp.float32))
    hidden = jax.nn.gelu(pre).astype(jnp.bfloat16)
    slot_out = jnp.einsum('erh,ehd->erd', hidden.astype(jnp.float32), w_out.astype(jnp.float32)).astype(jnp.bfloat16)
    slot_out = slot_out.reshape(slot_total, CLIPS, width)
    slot_out_f = slot_out.astype(jnp.float32)
    mixed = jnp.einsum('cts,scd->ctd', mixing_b.astype(jnp.float32), slot_out_f).astype(jnp.bfloat16)
    mixing_grad = jnp.einsum('ctd,scd->cts', grad_f, slot_out_f)
    slot_grad = jnp.einsum('cts,ctd->scd', mixing_b.astype(jnp.float32), grad_f).astype(jnp.bfloat16)
    grad_rows = slot_grad.reshape(experts, SLOTS * CLIPS, width).astype(jnp.float32)
    hidden_grad = jnp.einsum('erd,ehd->erh', grad_rows, w_out.astype(jnp.float32))
    pre_grad = jax.vjp(jax.nn.gelu, pre)[1](hidden_grad)[0].astype(jnp.bfloat16)
    pre_grad_f = pre_grad.astype(jnp.float32)
    grad_w_out = jnp.einsum('erh,erd->ehd', hidden.astype(jnp.float32), grad_rows).astype(jnp.bfloat16)
    grad_w_in = jnp.einsum('erd,erh->edh', expert_rows.astype(jnp.float32), pre_grad_f).astype(jnp.bfloat16)
    slot_in_grad = jnp.einsum('erh,edh->erd', pre_grad_f, w_in.astype(jnp.float32)).astype(jnp.bfloat16)
    slot_in_grad = slot_in_grad.reshape(slot_total, CLIPS, width).astype(jnp.float32)
    dispatch_grad = jnp.einsum('ctd,scd->cts', tokens_f, slot_in_grad)
    inner = lax.optimization_barrier(jnp.sum(dispatch * dispatch_grad, axis=1, keepdims=True))
    logit_grad = dispatch * (dispatch_grad - inner) + mixing * (mixing_grad - lax.optimization_barrier(jnp.sum(mixing * mixing_grad, axis=2, keepdims=True)))
    logit_b = logit_grad.astype(jnp.bfloat16)
    token_part = jnp.einsum('cts,scd->ctd', dispatch_b.astype(jnp.float32), slot_in_grad)
    router_part = jnp.dot(logit_b.reshape(CLIPS * TOKENS, slot_total).astype(jnp.float32), router.T.astype(jnp.float32), preferred_element_type=jnp.float32).reshape(CLIPS, TOKENS, width)
    grad_tokens = (token_part + router_part).astype(jnp.bfloat16)
    grad_router = jnp.einsum('ctd,cts->ds', tokens_f, logit_b.astype(jnp.float32))
    return (mixed, grad_tokens, grad_router, grad_w_in, grad_w_out)
```

```python
import functools

import jax
import jax.numpy as jnp
from jax import lax
from jax.experimental import pallas as pl
from jax.experimental.pallas import tpu as pltpu
from jax.sharding import PartitionSpec as P

MESH = pl.DeviceIdType.MESH
F32 = jnp.float32
BF16 = jnp.bfloat16
NT = (((1,), (1,)), ((), ()))
VMEM_BYTES = 67043328


def dot(a, b):
    return jnp.dot(a, b, preferred_element_type=F32)


def dot_nt(a, b):
    return lax.dot_general(a, b, NT, preferred_element_type=F32)


def place(seq_n, exp_n):
    s = lax.axis_index("seq")
    e = lax.axis_index("exp")
    half = exp_n // 2
    h, par = e // 2, e % 2
    pair = (s, h * 2 + (1 - par))
    seq_peers = [((s + k) % seq_n, e) for k in range(1, seq_n)]
    exp_peers = [(s, ((h + k) % half) * 2 + par) for k in range(1, half)]
    there = [((s + a) % seq_n, (h + b) % half) for a in range(seq_n) for b in range(half) if a or b]
    return s, h, par, pair, seq_peers, exp_peers, there


class Sender:
    def __init__(self, send_sem, recv_sem):
        self.send_sem, self.recv_sem, self.count, self.open = send_sem, recv_sem, 0, []

    def start(self, src, dst, peer):
        copy = pltpu.make_async_remote_copy(
            src_ref=src,
            dst_ref=dst,
            send_sem=self.send_sem.at[self.count],
            recv_sem=self.recv_sem.at[self.count],
            device_id=peer,
            device_id_type=MESH,
        )
        copy.start()
        self.count += 1
        self.open.append(copy)
        return copy

    def drain(self):
        for copy in self.open:
            copy.wait_send()


def copies_of(seq_n, exp_n):
    half = exp_n // 2
    reduce = 3 + 3 * (half - 1) + 3 * (seq_n - 1)
    gather = 2 * (seq_n - 1) + 4 * (half - 1) + 4 * half
    return reduce + gather + seq_n * half


def arrived(copies):
    for copy in copies:
        copy.wait_recv()


def stat_tile(*columns):
    shape = columns[0].shape[:-1] + (128,)
    lane = lax.broadcasted_iota(jnp.int32, shape, len(shape) - 1)
    tile = jnp.zeros(shape, F32)
    for i, column in enumerate(columns):
        tile = jnp.where(lane == i, column, tile)
    return tile


def join(parts):
    peak = parts[0][0]
    for p, _ in parts[1:]:
        peak = jnp.maximum(peak, p)
    factors = [jnp.exp(p - peak) for p, _ in parts]
    mass = factors[0] * parts[0][1]
    for f, (_, m) in zip(factors[1:], parts[1:]):
        mass = mass + f * m
    return peak, mass, factors


def split_stats(tile):
    return tile[..., 0:1], tile[..., 1:2]


def layer(
    seq_n, exp_n, tok_hbm, rt_hbm, gout_hbm, win_hbm, wout_hbm,
    mixed, gt, gwin, gwout, gr_o,
    tok, gout, rt, win, wout, lg, qf, dsp, lm, xt, qt,
    buf_a, rcv_a, buf_b, rcv_b, xg, se, ag,
    st_a, st_p, st_b, st_z, st_c, sa,
    gr_a, gr_p, gr_b, gr_r,
    w_sem, send_sem, recv_sem,
):
    clips, rows, width = tok.shape
    slots = rt.shape[0]
    half = exp_n // 2
    owned = slots // exp_n
    nr = clips * owned
    experts = win.shape[0]
    s, h, par, pair, seq_peers, exp_peers, there = place(seq_n, exp_n)
    far_peers = [(t, g * 2 + par) for t, g in there]

    load_rt = pltpu.make_async_copy(rt_hbm, rt, w_sem.at[0])
    load_tok = [pltpu.make_async_copy(tok_hbm.at[c], tok.at[c], w_sem.at[1 + c]) for c in range(clips)]
    load_gout = [
        pltpu.make_async_copy(gout_hbm.at[c], gout.at[c], w_sem.at[1 + clips + c]) for c in range(clips)
    ]
    load_in = pltpu.make_async_copy(win_hbm, win, w_sem.at[1 + 2 * clips])
    load_out = pltpu.make_async_copy(wout_hbm, wout, w_sem.at[2 + 2 * clips])
    load_rt.start()
    for load in load_tok:
        load.start()
    barrier = pltpu.get_barrier_semaphore()
    for peer in [pair] + far_peers:
        pl.semaphore_signal(barrier, inc=1, device_id=peer, device_id_type=MESH)
    net = Sender(send_sem, recv_sem)

    load_rt.wait()
    peaks, masses = [], []
    for c in range(clips):
        load_tok[c].wait()
        load_gout[c].start()
        value = dot_nt(rt[...], tok[c])
        lg[c] = value
        peak = jnp.max(value, axis=1, keepdims=True)
        p = jnp.exp(value - peak)
        peaks.append(peak.reshape(exp_n, owned, 1))
        masses.append(jnp.sum(p, axis=1, keepdims=True).reshape(exp_n, owned, 1))
        xt[c] = p.astype(BF16)
        q = jnp.exp(value - jnp.max(value, axis=0, keepdims=True))
        q = q / jnp.sum(q, axis=0, keepdims=True)
        qf[c] = q
        qt[c] = q.astype(BF16)
    load_out.start()
    load_in.start()
    tile = stat_tile(jnp.concatenate(peaks, axis=1), jnp.concatenate(masses, axis=1))
    tile = tile.reshape(half, 2, nr, 128)
    for q in range(2):
        st_a[q] = tile[:, q]

    def lay_out(kind, values):
        for g in range(half):
            for q in range(2):
                at = (2 * g + q) * owned
                rows_ = [value[at : at + owned] for value in values]
                buf_a[kind, q, g] = jnp.concatenate(rows_, axis=0).astype(BF16)

    def to_pair(kind):
        return [net.start(buf_a.at[kind, 1 - par], rcv_a.at[kind], pair)]

    def to_exp(kind, factors=None):
        for g in range(half):
            mine = buf_a[kind, par, g].astype(F32)
            other = rcv_a[kind, g].astype(F32)
            if factors is not None:
                mine, other = mine * factors[0][g], other * factors[1][g]
            buf_b[kind, g] = (mine + other).astype(BF16)
        return [
            net.start(buf_b.at[kind, (h + 1 + k) % half], rcv_b.at[kind, k], peer)
            for k, peer in enumerate(exp_peers)
        ]

    def to_seq(kind, factors=None):
        parts = [buf_b[kind, h].astype(F32)] + [rcv_b[kind, k].astype(F32) for k in range(half - 1)]
        if factors is not None:
            parts = [part * f for part, f in zip(parts, factors)]
        total = parts[0]
        for part in parts[1:]:
            total = total + part
        xg[kind, s] = total.astype(BF16)
        return [net.start(xg.at[kind, s], xg.at[kind, s], peer) for peer in seq_peers]

    def seq_total(ref, kind, factors=None):
        total = None
        for t in range(seq_n):
            part = ref[kind, t].astype(F32)
            if factors is not None:
                part = part * factors[t]
            total = part if total is None else total + part
        return total

    pl.semaphore_wait(barrier, 1 + len(far_peers))
    stat = [net.start(st_a.at[1 - par], st_p, pair)]
    lay_out(0, [dot(xt[c], tok[c]) for c in range(clips)])
    inputs = to_pair(0)
    for load in load_gout:
        load.wait()
    lay_out(1, [dot(qt[c], gout[c]) for c in range(clips)])
    grads = to_pair(1)
    arrived(stat)
    peak, mass, fac = join([split_stats(st_a[par]), split_stats(st_p[...])])
    st_b[...] = stat_tile(peak, mass)
    stat = [net.start(st_b.at[(h + 1 + k) % half], st_z.at[k], peer) for k, peer in enumerate(exp_peers)]
    arrived(inputs)
    inputs = to_exp(0, fac)
    arrived(grads)
    grads = to_exp(1)
    arrived(stat)
    peak, mass, fac = join([split_stats(st_b[h])] + [split_stats(st_z[k]) for k in range(half - 1)])
    st_c[s] = stat_tile(peak, mass)
    stat = [net.start(st_c.at[s], st_c.at[s], peer) for peer in seq_peers]
    arrived(inputs)
    inputs = to_seq(0, fac)
    arrived(grads)
    grads = to_seq(1)
    arrived(stat)
    peak, mass, fac = join([split_stats(st_c[t]) for t in range(seq_n)])
    fac = [f / mass for f in fac]
    sa[0, h, par] = stat_tile(peak, mass)

    row = lax.broadcasted_iota(jnp.int32, (nr, 1), 0)
    expert_of = (row % owned) // (owned // experts)
    mask = [(expert_of == e).astype(F32) for e in range(experts)]
    load_out.wait()
    load_in.wait()
    arrived(inputs)
    x_rows = seq_total(xg, 0, fac)
    pre = 0.0
    for e in range(experts):
        pre = pre + dot((x_rows * mask[e]).astype(BF16), win[e])
    hidden, back = jax.vjp(jax.nn.gelu, pre)

    def share(kind, part):
        se[kind, s] = part.astype(BF16)
        return [net.start(se.at[kind, s], se.at[kind, s], peer) for peer in seq_peers]

    out_part = 0.0
    for e in range(experts):
        out_part = out_part + dot((hidden * mask[e]).astype(BF16), wout[e])
    forward = share(0, out_part)
    arrived(grads)
    g_rows = seq_total(xg, 1).astype(BF16)
    hidden_grad = 0.0
    for e in range(experts):
        hidden_grad = hidden_grad + dot_nt(g_rows, wout[e]) * mask[e]
    pre_grad = back(hidden_grad)[0]
    in_part = 0.0
    for e in range(experts):
        in_part = in_part + dot_nt((pre_grad * mask[e]).astype(BF16), win[e])
    backward = share(1, in_part)

    def send_piece(kind, peers, g, q):
        copies = []
        for peer in peers:
            at, st = ag.at[kind, g, q], sa.at[kind, g, q]
            copies.append([net.start(st, st, peer), net.start(at, at, peer)])
        return copies

    def make_piece(kind):
        piece = seq_total(se, kind).astype(BF16)
        ag[kind, h, par] = piece
        if kind == 1:
            sa[1, h, par] = stat_tile(jnp.sum(piece.astype(F32) * x_rows, axis=1, keepdims=True))
        along = send_piece(kind, exp_peers, h, par)
        across = send_piece(kind, [pair], h, par)
        return along, across

    def pass_on(kind, along, across):
        for k in range(half - 1):
            arrived(along[k])
            across += send_piece(kind, [pair], (h + half - 1 - k) % half, par)

    def weight_grad(out, e, left, right):
        out[e] = dot((left * mask[e]).T.astype(BF16), right).astype(BF16)

    weight_grad(gwout, 0, hidden, g_rows)
    arrived(forward)
    along0, across0 = make_piece(0)
    for e in range(1, experts):
        weight_grad(gwout, e, hidden, g_rows)
    arrived(backward)
    along1, across1 = make_piece(1)
    pg = pre_grad.astype(BF16)
    for e in range(experts):
        weight_grad(gwin, e, x_rows, pg)
    pass_on(0, along0, across0)

    def of_clip(value, c):
        return value.reshape(exp_n, clips, owned, value.shape[-1])[:, c].reshape(slots, value.shape[-1])

    def spread(value, c):
        value = value.reshape(exp_n, 1, owned, value.shape[-1])
        zero = jnp.zeros_like(value)
        parts = [value if k == c else zero for k in range(clips)]
        return jnp.concatenate(parts, axis=1).reshape(clips * slots, value.shape[-1])

    for step in across0:
        arrived(step)
    so = ag[0].reshape(exp_n * nr, width)
    stats = sa[0].reshape(exp_n * nr, 128)
    for c in range(clips):
        mixing = qf[c]
        mixing_grad = of_clip(dot_nt(so, gout[c]), c)
        lm[c] = mixing * (mixing_grad - jnp.sum(mixing * mixing_grad, axis=0, keepdims=True))
        mine = of_clip(stats, c)
        dsp[c] = jnp.exp(lg[c] - mine[:, 0:1]) / mine[:, 1:2]
    pass_on(1, along1, across1)
    for c in range(clips):
        mixed[c] = dot(spread(qf[c], c).T.astype(BF16), so).astype(BF16)
    for step in across1:
        arrived(step)
    sig = ag[1].reshape(exp_n * nr, width)
    inner = sa[1].reshape(exp_n * nr, 128)
    gr = 0.0
    for c in range(clips):
        dispatch_grad = of_clip(dot_nt(sig, tok[c]), c)
        lgrad = dsp[c] * (dispatch_grad - of_clip(inner, c)[:, 0:1]) + lm[c]
        lm[c] = lgrad
        gr = gr + dot(lgrad.astype(BF16), tok[c])

    out_rows = gr_o.shape[0]
    packed = gr_b.shape[2]
    pack = out_rows // packed
    whole = gr.T
    for t in range(seq_n):
        for g in range(half):
            for q in range(2):
                at = (t * exp_n + 2 * g + q) * out_rows
                parts = [whole[at + j * packed : at + (j + 1) * packed] for j in range(pack)]
                gr_a[q, t, g] = jnp.concatenate(parts, axis=1).astype(BF16)
    last = [net.start(gr_a.at[1 - par], gr_p, pair)]
    both = jnp.concatenate([rt[...], sig], axis=0)

    def token_grad(c):
        left = jnp.concatenate([lm[c], spread(dsp[c], c)], axis=0)
        gt[c] = dot(left.T.astype(BF16), both).astype(BF16)

    arrived(last)
    gr_b[...] = (gr_a[par].astype(F32) + gr_p[...].astype(F32)).astype(BF16)
    last = [net.start(gr_b.at[t, g], gr_r.at[k], far_peers[k]) for k, (t, g) in enumerate(there)]
    for c in range(clips):
        token_grad(c)
    total = gr_b[s, h].astype(F32)
    for k, copy in enumerate(last):
        copy.wait_recv()
        total = total + gr_r[k].astype(F32)
    for j in range(pack):
        gr_o[j * packed : (j + 1) * packed] = total[:, j * slots : (j + 1) * slots]
    net.drain()


def put_out(n, *refs):
    ins, outs, sem = refs[:n], refs[n : 2 * n], refs[2 * n]
    copies = []
    for src, dst in zip(ins, outs):
        copies.append(pltpu.make_async_copy(src, dst, sem.at[len(copies)]))
        copies[-1].start()
    for copy in copies:
        copy.wait()


def on_device(seq_n, exp_n, tokens, router, w_in, w_out, grad_out):
    clips, rows, width = tokens.shape
    slots = router.shape[1]
    half = exp_n // 2
    owned = slots // exp_n
    nr = clips * owned
    vmem = pl.BlockSpec(memory_space=pltpu.VMEM)
    hbm = pl.BlockSpec(memory_space=pltpu.HBM)
    anywhere = pl.BlockSpec(memory_space=pl.ANY)
    shape = jax.ShapeDtypeStruct
    out_rows = width // (seq_n * exp_n)
    pack = max(1, 128 // slots)
    tile = (out_rows // pack, slots * pack)
    piece = (nr, width)
    stat = (nr, 128)
    n_copies = copies_of(seq_n, exp_n)
    outs = (
        shape(tokens.shape, BF16),
        shape(tokens.shape, BF16),
        shape(w_in.shape, BF16),
        shape(w_out.shape, BF16),
        shape((out_rows, slots), F32),
    )
    out_bytes = sum(o.size * o.dtype.itemsize for o in outs)
    limit = 30 * 2**20
    results = pl.pallas_call(
        functools.partial(layer, seq_n, exp_n),
        out_shape=outs,
        in_specs=[hbm] * 5,
        out_specs=(vmem,) * 5,
        scratch_shapes=[
            pltpu.VMEM(tokens.shape, BF16),
            pltpu.VMEM(tokens.shape, BF16),
            pltpu.VMEM((slots, width), BF16),
            pltpu.VMEM(w_in.shape, BF16),
            pltpu.VMEM(w_out.shape, BF16),
            pltpu.VMEM((clips, slots, rows), F32),
            pltpu.VMEM((clips, slots, rows), F32),
            pltpu.VMEM((clips, slots, rows), F32),
            pltpu.VMEM((clips, slots, rows), F32),
            pltpu.VMEM((clips, slots, rows), BF16),
            pltpu.VMEM((clips, slots, rows), BF16),
            pltpu.VMEM((2, 2, half) + piece, BF16),
            pltpu.VMEM((2, half) + piece, BF16),
            pltpu.VMEM((2, half) + piece, BF16),
            pltpu.VMEM((2, half - 1) + piece, BF16),
            pltpu.VMEM((2, seq_n) + piece, BF16),
            pltpu.VMEM((2, seq_n) + piece, BF16),
            pltpu.VMEM((2, half, 2) + piece, BF16),
            pltpu.VMEM((2, half) + stat, F32),
            pltpu.VMEM((half,) + stat, F32),
            pltpu.VMEM((half,) + stat, F32),
            pltpu.VMEM((half - 1,) + stat, F32),
            pltpu.VMEM((seq_n,) + stat, F32),
            pltpu.VMEM((2, half, 2) + stat, F32),
            pltpu.VMEM((2, seq_n, half) + tile, BF16),
            pltpu.VMEM((seq_n, half) + tile, BF16),
            pltpu.VMEM((seq_n, half) + tile, BF16),
            pltpu.VMEM((seq_n * half - 1,) + tile, BF16),
            pltpu.SemaphoreType.DMA((2 * clips + 3,)),
            pltpu.SemaphoreType.DMA((n_copies,)),
            pltpu.SemaphoreType.DMA((n_copies,)),
        ],
        compiler_params=pltpu.CompilerParams(
            collective_id=0, has_side_effects=True, vmem_limit_bytes=limit
        ),
        name="layer",
    )(tokens, router.T, grad_out, w_in, w_out)
    mixed, grad_tokens, grad_w_in, grad_w_out, grad_router = pl.pallas_call(
        functools.partial(put_out, len(outs)),
        out_shape=outs,
        in_specs=[anywhere] * len(outs),
        out_specs=(hbm,) * len(outs),
        scratch_shapes=[pltpu.SemaphoreType.DMA((len(outs),))],
        compiler_params=pltpu.CompilerParams(vmem_limit_bytes=2**20),
        name="put_out",
    )(*results)
    return mixed, grad_tokens, grad_router, grad_w_in, grad_w_out


def solution(mesh):
    return jax.shard_map(
        functools.partial(on_device, mesh.shape["seq"], mesh.shape["exp"]),
        mesh=mesh,
        in_specs=(
            P(None, ("seq", "exp"), None),
            P(),
            P("exp", None, "seq"),
            P("exp", "seq", None),
            P(None, ("seq", "exp"), None),
        ),
        out_specs=(
            P(None, ("seq", "exp"), None),
            P(None, ("seq", "exp"), None),
            P(("seq", "exp"), None),
            P("exp", None, "seq"),
            P("exp", "seq", None),
        ),
        check_vma=False,
    )
```

```python
import functools

import jax
import jax.numpy as jnp
from jax import lax
from jax.experimental import pallas as pl
from jax.experimental.pallas import tpu as pltpu
from jax.sharding import PartitionSpec as P

MESH = pl.DeviceIdType.MESH
F32 = jnp.float32
BF16 = jnp.bfloat16
NT = (((1,), (1,)), ((), ()))
VMEM_BYTES = 67043328


def dot(a, b):
    return jnp.dot(a, b, preferred_element_type=F32)


def dot_nt(a, b):
    return lax.dot_general(a, b, NT, preferred_element_type=F32)


def place(seq_n, exp_n):
    s = lax.axis_index("seq")
    e = lax.axis_index("exp")
    half = exp_n // 2
    h, par = e // 2, e % 2
    pair = (s, h * 2 + (1 - par))
    seq_peers = [((s + k) % seq_n, e) for k in range(1, seq_n)]
    exp_peers = [(s, ((h + k) % half) * 2 + par) for k in range(1, half)]
    there = [((s + a) % seq_n, (h + b) % half) for a in range(seq_n) for b in range(half) if a or b]
    return s, h, par, pair, seq_peers, exp_peers, there


class Sender:
    def __init__(self, send_sem, recv_sem):
        self.send_sem, self.recv_sem, self.count, self.open = send_sem, recv_sem, 0, []

    def start(self, src, dst, peer):
        copy = pltpu.make_async_remote_copy(
            src_ref=src,
            dst_ref=dst,
            send_sem=self.send_sem.at[self.count],
            recv_sem=self.recv_sem.at[self.count],
            device_id=peer,
            device_id_type=MESH,
        )
        copy.start()
        self.count += 1
        self.open.append(copy)
        return copy

    def drain(self):
        for copy in self.open:
            copy.wait_send()


def copies_of(seq_n, exp_n):
    half = exp_n // 2
    reduce = 3 + 3 * (half - 1) + 3 * (seq_n - 1)
    gather = 2 * (seq_n - 1) + 4 * (half - 1) + 4 * half
    return reduce + gather + seq_n * half


def arrived(copies):
    for copy in copies:
        copy.wait_recv()


def stat_tile(*columns):
    shape = columns[0].shape[:-1] + (128,)
    lane = lax.broadcasted_iota(jnp.int32, shape, len(shape) - 1)
    tile = jnp.zeros(shape, F32)
    for i, column in enumerate(columns):
        tile = jnp.where(lane == i, column, tile)
    return tile


def join(parts):
    peak = parts[0][0]
    for p, _ in parts[1:]:
        peak = jnp.maximum(peak, p)
    factors = [jnp.exp(p - peak) for p, _ in parts]
    mass = factors[0] * parts[0][1]
    for f, (_, m) in zip(factors[1:], parts[1:]):
        mass = mass + f * m
    return peak, mass, factors


def split_stats(tile):
    return tile[..., 0:1], tile[..., 1:2]


def layer(
    seq_n, exp_n, tok_hbm, rt_hbm, gout_hbm, win_hbm, wout_hbm,
    mixed, gt, gwin, gwout, gr_o,
    tok, gout, rt, win, wout, lg, qf, dsp, lm, xt, qt,
    buf_a, rcv_a, buf_b, rcv_b, xg, se, ag,
    st_a, st_p, st_b, st_z, st_c, sa,
    gr_a, gr_p, gr_b, gr_r,
    w_sem, send_sem, recv_sem,
):
    clips, rows, width = tok.shape
    slots = rt.shape[0]
    half = exp_n // 2
    owned = slots // exp_n
    nr = clips * owned
    experts = win.shape[0]
    s, h, par, pair, seq_peers, exp_peers, there = place(seq_n, exp_n)
    far_peers = [(t, g * 2 + par) for t, g in there]

    load_rt = pltpu.make_async_copy(rt_hbm, rt, w_sem.at[0])
    load_tok = [pltpu.make_async_copy(tok_hbm.at[c], tok.at[c], w_sem.at[1 + c]) for c in range(clips)]
    load_gout = [
        pltpu.make_async_copy(gout_hbm.at[c], gout.at[c], w_sem.at[1 + clips + c]) for c in range(clips)
    ]
    load_in = pltpu.make_async_copy(win_hbm, win, w_sem.at[1 + 2 * clips])
    load_out = pltpu.make_async_copy(wout_hbm, wout, w_sem.at[2 + 2 * clips])
    load_rt.start()
    for load in load_tok:
        load.start()
    barrier = pltpu.get_barrier_semaphore()
    for peer in [pair] + far_peers:
        pl.semaphore_signal(barrier, inc=1, device_id=peer, device_id_type=MESH)
    net = Sender(send_sem, recv_sem)

    load_rt.wait()
    peaks, masses = [], []
    for c in range(clips):
        load_tok[c].wait()
        load_gout[c].start()
        value = dot_nt(rt[...], tok[c])
        lg[c] = value
        peak = jnp.max(value, axis=1, keepdims=True)
        p = jnp.exp(value - peak)
        peaks.append(peak.reshape(exp_n, owned, 1))
        masses.append(jnp.sum(p, axis=1, keepdims=True).reshape(exp_n, owned, 1))
        xt[c] = p.astype(BF16)
        q = jnp.exp(value - jnp.max(value, axis=0, keepdims=True))
        q = q / jnp.sum(q, axis=0, keepdims=True)
        qf[c] = q
        qt[c] = q.astype(BF16)
    load_out.start()
    load_in.start()
    tile = stat_tile(jnp.concatenate(peaks, axis=1), jnp.concatenate(masses, axis=1))
    tile = tile.reshape(half, 2, nr, 128)
    for q in range(2):
        st_a[q] = tile[:, q]

    def lay_out(kind, values):
        for g in range(half):
            for q in range(2):
                at = (2 * g + q) * owned
                rows_ = [value[at : at + owned] for value in values]
                buf_a[kind, q, g] = jnp.concatenate(rows_, axis=0).astype(BF16)

    def to_pair(kind):
        return [net.start(buf_a.at[kind, 1 - par], rcv_a.at[kind], pair)]

    def to_exp(kind, factors=None):
        for g in range(half):
            mine = buf_a[kind, par, g].astype(F32)
            other = rcv_a[kind, g].astype(F32)
            if factors is not None:
                mine, other = mine * factors[0][g], other * factors[1][g]
            buf_b[kind, g] = (mine + other).astype(BF16)
        return [
            net.start(buf_b.at[kind, (h + 1 + k) % half], rcv_b.at[kind, k], peer)
            for k, peer in enumerate(exp_peers)
        ]

    def to_seq(kind, factors=None):
        parts = [buf_b[kind, h].astype(F32)] + [rcv_b[kind, k].astype(F32) for k in range(half - 1)]
        if factors is not None:
            parts = [part * f for part, f in zip(parts, factors)]
        total = parts[0]
        for part in parts[1:]:
            total = total + part
        xg[kind, s] = total.astype(BF16)
        return [net.start(xg.at[kind, s], xg.at[kind, s], peer) for peer in seq_peers]

    def seq_total(ref, kind, factors=None):
        total = None
        for t in range(seq_n):
            part = ref[kind, t].astype(F32)
            if factors is not None:
                part = part * factors[t]
            total = part if total is None else total + part
        return total

    pl.semaphore_wait(barrier, 1 + len(far_peers))
    stat = [net.start(st_a.at[1 - par], st_p, pair)]
    lay_out(0, [dot(xt[c], tok[c]) for c in range(clips)])
    inputs = to_pair(0)
    for load in load_gout:
        load.wait()
    lay_out(1, [dot(qt[c], gout[c]) for c in range(clips)])
    grads = to_pair(1)
    arrived(stat)
    peak, mass, fac = join([split_stats(st_a[par]), split_stats(st_p[...])])
    st_b[...] = stat_tile(peak, mass)
    stat = [net.start(st_b.at[(h + 1 + k) % half], st_z.at[k], peer) for k, peer in enumerate(exp_peers)]
    arrived(inputs)
    inputs = to_exp(0, fac)
    arrived(grads)
    grads = to_exp(1)
    arrived(stat)
    peak, mass, fac = join([split_stats(st_b[h])] + [split_stats(st_z[k]) for k in range(half - 1)])
    st_c[s] = stat_tile(peak, mass)
    stat = [net.start(st_c.at[s], st_c.at[s], peer) for peer in seq_peers]
    arrived(inputs)
    inputs = to_seq(0, fac)
    arrived(grads)
    grads = to_seq(1)
    arrived(stat)
    peak, mass, fac = join([split_stats(st_c[t]) for t in range(seq_n)])
    fac = [f / mass for f in fac]
    sa[0, h, par] = stat_tile(peak, mass)

    row = lax.broadcasted_iota(jnp.int32, (nr, 1), 0)
    expert_of = (row % owned) // (owned // experts)
    mask = [(expert_of == e).astype(F32) for e in range(experts)]
    load_out.wait()
    load_in.wait()
    arrived(inputs)
    x_rows = seq_total(xg, 0, fac)
    pre = 0.0
    for e in range(experts):
        pre = pre + dot((x_rows * mask[e]).astype(BF16), win[e])
    hidden, back = jax.vjp(jax.nn.gelu, pre)

    def share(kind, part):
        se[kind, s] = part.astype(BF16)
        return [net.start(se.at[kind, s], se.at[kind, s], peer) for peer in seq_peers]

    out_part = 0.0
    for e in range(experts):
        out_part = out_part + dot((hidden * mask[e]).astype(BF16), wout[e])
    forward = share(0, out_part)
    arrived(grads)
    g_rows = seq_total(xg, 1).astype(BF16)
    hidden_grad = 0.0
    for e in range(experts):
        hidden_grad = hidden_grad + dot_nt(g_rows, wout[e]) * mask[e]
    pre_grad = back(hidden_grad)[0]
    in_part = 0.0
    for e in range(experts):
        in_part = in_part + dot_nt((pre_grad * mask[e]).astype(BF16), win[e])
    backward = share(1, in_part)

    def send_piece(kind, peers, g, q):
        copies = []
        for peer in peers:
            at, st = ag.at[kind, g, q], sa.at[kind, g, q]
            copies.append([net.start(st, st, peer), net.start(at, at, peer)])
        return copies

    def make_piece(kind):
        piece = seq_total(se, kind).astype(BF16)
        ag[kind, h, par] = piece
        if kind == 1:
            sa[1, h, par] = stat_tile(jnp.sum(piece.astype(F32) * x_rows, axis=1, keepdims=True))
        along = send_piece(kind, exp_peers, h, par)
        across = send_piece(kind, [pair], h, par)
        return along, across

    def pass_on(kind, along, across):
        for k in range(half - 1):
            arrived(along[k])
            across += send_piece(kind, [pair], (h + half - 1 - k) % half, par)

    def weight_grad(out, e, left, right):
        out[e] = dot((left * mask[e]).T.astype(BF16), right).astype(BF16)

    weight_grad(gwout, 0, hidden, g_rows)
    arrived(forward)
    along0, across0 = make_piece(0)
    for e in range(1, experts):
        weight_grad(gwout, e, hidden, g_rows)
    arrived(backward)
    along1, across1 = make_piece(1)
    pg = pre_grad.astype(BF16)
    for e in range(experts):
        weight_grad(gwin, e, x_rows, pg)
    pass_on(0, along0, across0)

    def of_clip(value, c):
        return value.reshape(exp_n, clips, owned, value.shape[-1])[:, c].reshape(slots, value.shape[-1])

    def spread(value, c):
        value = value.reshape(exp_n, 1, owned, value.shape[-1])
        zero = jnp.zeros_like(value)
        parts = [value if k == c else zero for k in range(clips)]
        return jnp.concatenate(parts, axis=1).reshape(clips * slots, value.shape[-1])

    for step in across0:
        arrived(step)
    so = ag[0].reshape(exp_n * nr, width)
    stats = sa[0].reshape(exp_n * nr, 128)
    for c in range(clips):
        mixing = qf[c]
        mixing_grad = of_clip(dot_nt(so, gout[c]), c)
        lm[c] = mixing * (mixing_grad - jnp.sum(mixing * mixing_grad, axis=0, keepdims=True))
        mine = of_clip(stats, c)
        dsp[c] = jnp.exp(lg[c] - mine[:, 0:1]) / mine[:, 1:2]
    pass_on(1, along1, across1)
    for c in range(clips):
        mixed[c] = dot(spread(qf[c], c).T.astype(BF16), so).astype(BF16)
    for step in across1:
        arrived(step)
    sig = ag[1].reshape(exp_n * nr, width)
    inner = sa[1].reshape(exp_n * nr, 128)
    gr = 0.0
    for c in range(clips):
        dispatch_grad = of_clip(dot_nt(sig, tok[c]), c)
        lgrad = dsp[c] * (dispatch_grad - of_clip(inner, c)[:, 0:1]) + lm[c]
        lm[c] = lgrad
        gr = gr + dot(lgrad.astype(BF16), tok[c])

    out_rows = gr_o.shape[0]
    packed = gr_b.shape[2]
    pack = out_rows // packed
    whole = gr.T
    for t in range(seq_n):
        for g in range(half):
            for q in range(2):
                at = (t * exp_n + 2 * g + q) * out_rows
                parts = [whole[at + j * packed : at + (j + 1) * packed] for j in range(pack)]
                gr_a[q, t, g] = jnp.concatenate(parts, axis=1).astype(BF16)
    last = [net.start(gr_a.at[1 - par], gr_p, pair)]
    both = jnp.concatenate([rt[...], sig], axis=0)

    def token_grad(c):
        left = jnp.concatenate([lm[c], spread(dsp[c], c)], axis=0)
        gt[c] = dot(left.T.astype(BF16), both).astype(BF16)

    arrived(last)
    gr_b[...] = (gr_a[par].astype(F32) + gr_p[...].astype(F32)).astype(BF16)
    last = [net.start(gr_b.at[t, g], gr_r.at[k], far_peers[k]) for k, (t, g) in enumerate(there)]
    for c in range(clips):
        token_grad(c)
    total = gr_b[s, h].astype(F32)
    for k, copy in enumerate(last):
        copy.wait_recv()
        total = total + gr_r[k].astype(F32)
    for j in range(pack):
        gr_o[j * packed : (j + 1) * packed] = total[:, j * slots : (j + 1) * slots]
    net.drain()


def put_out(n, *refs):
    ins, outs, sem = refs[:n], refs[n : 2 * n], refs[2 * n]
    copies = []
    for src, dst in zip(ins, outs):
        copies.append(pltpu.make_async_copy(src, dst, sem.at[len(copies)]))
        copies[-1].start()
    for copy in copies:
        copy.wait()


def on_device(seq_n, exp_n, tokens, router, w_in, w_out, grad_out):
    clips, rows, width = tokens.shape
    slots = router.shape[1]
    half = exp_n // 2
    owned = slots // exp_n
    nr = clips * owned
    vmem = pl.BlockSpec(memory_space=pltpu.VMEM)
    hbm = pl.BlockSpec(memory_space=pltpu.HBM)
    anywhere = pl.BlockSpec(memory_space=pl.ANY)
    shape = jax.ShapeDtypeStruct
    out_rows = width // (seq_n * exp_n)
    pack = max(1, 128 // slots)
    tile = (out_rows // pack, slots * pack)
    piece = (nr, width)
    stat = (nr, 128)
    n_copies = copies_of(seq_n, exp_n)
    outs = (
        shape(tokens.shape, BF16),
        shape(tokens.shape, BF16),
        shape(w_in.shape, BF16),
        shape(w_out.shape, BF16),
        shape((out_rows, slots), F32),
    )
    limit = VMEM_BYTES // 2
    results = pl.pallas_call(
        functools.partial(layer, seq_n, exp_n),
        out_shape=outs,
        in_specs=[hbm] * 5,
        out_specs=(vmem,) * 5,
        scratch_shapes=[
            pltpu.VMEM(tokens.shape, BF16),
            pltpu.VMEM(tokens.shape, BF16),
            pltpu.VMEM((slots, width), BF16),
            pltpu.VMEM(w_in.shape, BF16),
            pltpu.VMEM(w_out.shape, BF16),
            pltpu.VMEM((clips, slots, rows), F32),
            pltpu.VMEM((clips, slots, rows), F32),
            pltpu.VMEM((clips, slots, rows), F32),
            pltpu.VMEM((clips, slots, rows), F32),
            pltpu.VMEM((clips, slots, rows), BF16),
            pltpu.VMEM((clips, slots, rows), BF16),
            pltpu.VMEM((2, 2, half) + piece, BF16),
            pltpu.VMEM((2, half) + piece, BF16),
            pltpu.VMEM((2, half) + piece, BF16),
            pltpu.VMEM((2, half - 1) + piece, BF16),
            pltpu.VMEM((2, seq_n) + piece, BF16),
            pltpu.VMEM((2, seq_n) + piece, BF16),
            pltpu.VMEM((2, half, 2) + piece, BF16),
            pltpu.VMEM((2, half) + stat, F32),
            pltpu.VMEM((half,) + stat, F32),
            pltpu.VMEM((half,) + stat, F32),
            pltpu.VMEM((half - 1,) + stat, F32),
            pltpu.VMEM((seq_n,) + stat, F32),
            pltpu.VMEM((2, half, 2) + stat, F32),
            pltpu.VMEM((2, seq_n, half) + tile, BF16),
            pltpu.VMEM((seq_n, half) + tile, BF16),
            pltpu.VMEM((seq_n, half) + tile, BF16),
            pltpu.VMEM((seq_n * half - 1,) + tile, BF16),
            pltpu.SemaphoreType.DMA((2 * clips + 3,)),
            pltpu.SemaphoreType.DMA((n_copies,)),
            pltpu.SemaphoreType.DMA((n_copies,)),
        ],
        compiler_params=pltpu.CompilerParams(
            collective_id=0, has_side_effects=True, vmem_limit_bytes=limit
        ),
        name="layer",
    )(*[pltpu.with_memory_space_constraint(a, pltpu.HBM) for a in (tokens, router.T, grad_out, w_in, w_out)])
    mixed, grad_tokens, grad_w_in, grad_w_out, grad_router = pl.pallas_call(
        functools.partial(put_out, len(outs)),
        out_shape=outs,
        in_specs=[anywhere] * len(outs),
        out_specs=(hbm,) * len(outs),
        scratch_shapes=[pltpu.SemaphoreType.DMA((len(outs),))],
        compiler_params=pltpu.CompilerParams(vmem_limit_bytes=2**20),
        name="put_out",
    )(*results)
    return mixed, grad_tokens, grad_router, grad_w_in, grad_w_out


def solution(mesh):
    return jax.shard_map(
        functools.partial(on_device, mesh.shape["seq"], mesh.shape["exp"]),
        mesh=mesh,
        in_specs=(
            P(None, ("seq", "exp"), None),
            P(),
            P("exp", None, "seq"),
            P("exp", "seq", None),
            P(None, ("seq", "exp"), None),
        ),
        out_specs=(
            P(None, ("seq", "exp"), None),
            P(None, ("seq", "exp"), None),
            P(("seq", "exp"), None),
            P("exp", None, "seq"),
            P("exp", "seq", None),
        ),
        check_vma=False,
    )
```

```python
import functools

import jax
import jax.numpy as jnp
from jax import lax
from jax.experimental import pallas as pl
from jax.experimental.pallas import tpu as pltpu
from jax.sharding import PartitionSpec as P

MESH = pl.DeviceIdType.MESH
F32 = jnp.float32
BF16 = jnp.bfloat16
NT = (((1,), (1,)), ((), ()))
VMEM_BYTES = 67043328


def dot(a, b):
    return jnp.dot(a, b, preferred_element_type=F32)


def dot_nt(a, b):
    return lax.dot_general(a, b, NT, preferred_element_type=F32)


def place(seq_n, exp_n):
    s = lax.axis_index("seq")
    e = lax.axis_index("exp")
    half = exp_n // 2
    h, par = e // 2, e % 2
    pair = (s, h * 2 + (1 - par))
    seq_peers = [((s + k) % seq_n, e) for k in range(1, seq_n)]
    exp_peers = [(s, ((h + k) % half) * 2 + par) for k in range(1, half)]
    there = [((s + a) % seq_n, (h + b) % half) for a in range(seq_n) for b in range(half) if a or b]
    return s, h, par, pair, seq_peers, exp_peers, there


class Net:
    def __init__(self, send_sem, recv_sem):
        self.send_sem, self.recv_sem, self.groups = send_sem, recv_sem, []

    def group(self, whole):
        self.groups.append(whole)
        return Group(self, len(self.groups) - 1, whole)

    def drain(self):
        for i, whole in enumerate(self.groups):
            pltpu.make_async_copy(whole, whole, self.send_sem.at[i]).wait()


class Group:
    def __init__(self, net, index, whole):
        self.net, self.index, self.whole = net, index, whole

    def start(self, src, dst, peer):
        pltpu.make_async_remote_copy(
            src_ref=src,
            dst_ref=dst,
            send_sem=self.net.send_sem.at[self.index],
            recv_sem=self.net.recv_sem.at[self.index],
            device_id=peer,
            device_id_type=MESH,
        ).start()
        return self

    def show(self, peers, ref, *at):
        for peer in peers:
            self.start(ref.at[at], ref.at[at], peer)
        return self

    def arrived(self):
        pltpu.make_async_copy(self.whole, self.whole, self.net.recv_sem.at[self.index]).wait()


def groups_of(seq_n, exp_n):
    return 21 + (seq_n - 1) + (exp_n // 2 - 1)


def stat_tile(columns):
    shape = columns[0].shape[:-1] + (128,)
    lane = lax.broadcasted_iota(jnp.int32, shape, len(shape) - 1)
    tile = jnp.zeros(shape, F32)
    for i, column in enumerate(columns):
        tile = jnp.where(lane == i, column, tile)
    return tile


def by_clip(column, clips):
    owned = column.shape[-2] // clips
    return [column[..., c * owned : (c + 1) * owned, :] for c in range(clips)]


def split_stats(tile, clips):
    lanes = [tile[..., i : i + 1] for i in range(2 * clips)]
    axis = len(tile.shape) - 2
    return jnp.concatenate(lanes[:clips], axis=axis), jnp.concatenate(lanes[clips:], axis=axis)


def join(parts):
    peak = parts[0][0]
    for p, _ in parts[1:]:
        peak = jnp.maximum(peak, p)
    factors = [jnp.exp(p - peak) for p, _ in parts]
    mass = factors[0] * parts[0][1]
    for f, (_, m) in zip(factors[1:], parts[1:]):
        mass = mass + f * m
    return peak, mass, factors


def layer(
    seq_n, exp_n, tok_hbm, rt_hbm, gout_hbm, win_hbm, wout_hbm,
    mixed, gt, gwin, gwout, gr_o,
    tok, gout, rt, win, wout, lg, qf, dsp, lm, xt, qt,
    buf_a, rcv_a, xb, xr, xg, gb, gbr, gc, gcr, gg, fe, fer, se, so_ag, sig_ag,
    st_a, st_p, st_b, st_z, st_c, sa, si,
    gr_a, gr_p, gr_b, gr_r,
    w_sem, send_sem, recv_sem,
):
    clips, rows, width = tok.shape
    slots = rt.shape[0]
    half = exp_n // 2
    owned = slots // exp_n
    nr = clips * owned
    dc = width // seq_n
    experts = win.shape[0]
    s, h, par, pair, seq_peers, exp_peers, there = place(seq_n, exp_n)
    far_peers = [(t, g * 2 + par) for t, g in there]

    load_rt = pltpu.make_async_copy(rt_hbm, rt, w_sem.at[0])
    load_tok = [pltpu.make_async_copy(tok_hbm.at[c], tok.at[c], w_sem.at[1 + c]) for c in range(clips)]
    load_gout = [
        pltpu.make_async_copy(gout_hbm.at[c], gout.at[c], w_sem.at[1 + clips + c]) for c in range(clips)
    ]
    load_in = pltpu.make_async_copy(win_hbm, win, w_sem.at[1 + 2 * clips])
    load_out = pltpu.make_async_copy(wout_hbm, wout, w_sem.at[2 + 2 * clips])
    load_rt.start()
    for load in load_tok:
        load.start()
    barrier = pltpu.get_barrier_semaphore()
    for peer in [pair] + far_peers:
        pl.semaphore_signal(barrier, inc=1, device_id=peer, device_id_type=MESH)
    net = Net(send_sem, recv_sem)

    load_rt.wait()
    values, peaks, masses = [], [], []
    for c in range(clips):
        load_tok[c].wait()
        load_gout[c].start()
        values.append(dot_nt(rt[...], tok[c]))
    for c, value in enumerate(values):
        lg[c] = value
        peak = jnp.max(value, axis=1, keepdims=True)
        p = jnp.exp(value - peak)
        peaks.append(peak.reshape(half, 2, owned, 1))
        masses.append(jnp.sum(p, axis=1, keepdims=True).reshape(half, 2, owned, 1))
        xt[c] = p.astype(BF16)
    for c, value in enumerate(values):
        q = jnp.exp(value - jnp.max(value, axis=0, keepdims=True))
        q = q / jnp.sum(q, axis=0, keepdims=True)
        qf[c] = q
        qt[c] = q.astype(BF16)
    tile = stat_tile(peaks + masses)
    for q in range(2):
        st_a[q] = tile[:, q]

    def lay_out(kind, values):
        for g in range(half):
            for q in range(2):
                at = (2 * g + q) * owned
                rows_ = [value[at : at + owned] for value in values]
                buf_a[kind, q, g] = jnp.concatenate(rows_, axis=0).astype(BF16)

    def pair_sum(kind, g, factors=None):
        mine = buf_a[kind, par, g].astype(F32)
        other = rcv_a[kind, g].astype(F32)
        if factors is not None:
            mine, other = mine * factors[0][g], other * factors[1][g]
        return (mine + other).astype(BF16)

    def spread_over(peers, at, ref, dst):
        group = net.group(dst)
        for k, peer in enumerate(peers):
            group.start(ref.at[at(k)], dst.at[k], peer)
        return group

    def show_seq(ref):
        return net.group(ref.at[pl.ds(0, seq_n - 1)]).show(seq_peers, ref, s)

    def exp_of(k):
        return (h + 1 + k) % half

    def seq_of(k):
        return (s + 1 + k) % seq_n

    def add_up(parts, factors=None):
        parts = [part.astype(F32) for part in parts]
        if factors is not None:
            parts = [part * f for part, f in zip(parts, factors)]
        total = parts[0]
        for part in parts[1:]:
            total = total + part
        return total

    lay_out(0, [dot(xt[c], tok[c]) for c in range(clips)])
    pl.semaphore_wait(barrier, 1 + len(far_peers))
    stat = net.group(st_p).start(st_a.at[1 - par], st_p, pair)
    inputs = net.group(rcv_a.at[0]).start(buf_a.at[0, 1 - par], rcv_a.at[0], pair)
    for load in load_gout:
        load.wait()
    lay_out(1, [dot(qt[c], gout[c]) for c in range(clips)])
    grads = net.group(rcv_a.at[1]).start(buf_a.at[1, 1 - par], rcv_a.at[1], pair)
    load_out.start()
    load_in.start()

    stat.arrived()
    peak, mass, fac = join([split_stats(st_a[par], clips), split_stats(st_p[...], clips)])
    st_b[...] = stat_tile(by_clip(peak, clips) + by_clip(mass, clips))
    stat = spread_over(exp_peers, exp_of, st_b, st_z)
    inputs.arrived()
    for g in range(half):
        xb[g] = pair_sum(0, g, fac)
    inputs = spread_over(exp_peers, exp_of, xb, xr)
    grads.arrived()
    for g in range(half):
        value = pair_sum(1, g)
        for t in range(seq_n):
            gb[t, g] = value[:, t * dc : (t + 1) * dc]
    grads = spread_over(seq_peers, seq_of, gb, gbr)
    stat.arrived()
    parts = [split_stats(st_b[h], clips)] + [split_stats(st_z[k], clips) for k in range(half - 1)]
    peak, mass, fac = join(parts)
    st_c[s] = stat_tile(by_clip(peak, clips) + by_clip(mass, clips))
    stat = show_seq(st_c)
    grads.arrived()
    for g in range(half):
        gc[g] = add_up([gb[s, g]] + [gbr[k, g] for k in range(seq_n - 1)]).astype(BF16)
    grads = spread_over(exp_peers, exp_of, gc, gcr)
    inputs.arrived()
    xg[s] = add_up([xb[h]] + [xr[k] for k in range(half - 1)], fac).astype(BF16)
    inputs = show_seq(xg)
    stat.arrived()
    peak, mass, fac = join([split_stats(st_c[t], clips) for t in range(seq_n)])
    fac = [f / mass for f in fac]
    sa[h, par] = stat_tile(by_clip(peak, clips) + by_clip(mass, clips))
    stat_along = net.group(sa.at[pl.ds(0, half - 1), 0]).show(exp_peers, sa, h, par)
    stat_across = net.group(sa.at[pl.ds(0, half), 0]).show([pair], sa, h, par)
    grads.arrived()
    gg[s] = add_up([gc[h]] + [gcr[k] for k in range(half - 1)]).astype(BF16)
    grads = show_seq(gg)

    row = lax.broadcasted_iota(jnp.int32, (nr, 1), 0)
    expert_of = (row % owned) // (owned // experts)
    mask = [(expert_of == e).astype(F32) for e in range(experts)]
    load_out.wait()
    load_in.wait()
    inputs.arrived()
    x_rows = add_up([xg[t] for t in range(seq_n)], fac)
    pre = 0.0
    for e in range(experts):
        pre = pre + dot((x_rows * mask[e]).astype(BF16), win[e])
    hidden, back = jax.vjp(jax.nn.gelu, pre)
    out_part = 0.0
    for e in range(experts):
        out_part = out_part + dot((hidden * mask[e]).astype(BF16), wout[e])
    for t in range(seq_n):
        fe[t] = out_part[:, t * dc : (t + 1) * dc].astype(BF16)
    forward = spread_over(seq_peers, seq_of, fe, fer)
    grads.arrived()
    g_rows = jnp.concatenate([gg[t] for t in range(seq_n)], axis=1)
    hidden_grad = 0.0
    for e in range(experts):
        hidden_grad = hidden_grad + dot_nt(g_rows, wout[e]) * mask[e]
    pre_grad = back(hidden_grad)[0]
    in_part = 0.0
    for e in range(experts):
        in_part = in_part + dot_nt((pre_grad * mask[e]).astype(BF16), win[e])
    se[s] = in_part.astype(BF16)
    backward = show_seq(se)

    def from_exp(k):
        return (h + half - 1 - k) % half

    def weight_grad(out, e, left, right):
        out[e] = dot((left * mask[e]).T.astype(BF16), right).astype(BF16)

    forward.arrived()
    so_ag[par, s, h] = add_up([fe[s]] + [fer[k] for k in range(seq_n - 1)]).astype(BF16)
    forward = net.group(so_ag.at[0, 0, pl.ds(0, half - 1)]).show(exp_peers, so_ag, par, s, h)
    stat_along.arrived()
    for k in range(half - 1):
        stat_across.show([pair], sa, from_exp(k), par)
    for e in range(experts):
        weight_grad(gwout, e, hidden, g_rows)
    pg = pre_grad.astype(BF16)
    weight_grad(gwin, 0, x_rows, pg)
    forward.arrived()
    forward = [net.group(so_ag.at[0, 0]).show([peer], so_ag, par, s) for peer in seq_peers]
    columns = net.group(so_ag.at[0]).show([pair], so_ag, par, s)
    backward.arrived()
    piece = add_up([se[t] for t in range(seq_n)]).astype(BF16)
    sig_ag[h, par] = piece
    inner = jnp.sum(piece.astype(F32) * x_rows, axis=1, keepdims=True)
    si[h, par] = stat_tile(by_clip(inner, clips))
    along = [net.group(sig_ag.at[0, 0]).show([peer], sig_ag, h, par) for peer in exp_peers]
    inner_along = net.group(si.at[pl.ds(0, half - 1), 0]).show(exp_peers, si, h, par)
    across = net.group(sig_ag.at[pl.ds(0, half), 0]).show([pair], sig_ag, h, par)
    inner_across = net.group(si.at[pl.ds(0, half), 0]).show([pair], si, h, par)
    for e in range(1, experts):
        weight_grad(gwin, e, x_rows, pg)
    for k in range(seq_n - 1):
        forward[k].arrived()
        columns.show([pair], so_ag, par, (s + seq_n - 1 - k) % seq_n)
    for k in range(half - 1):
        along[k].arrived()
        across.show([pair], sig_ag, from_exp(k), par)
    inner_along.arrived()
    for k in range(half - 1):
        inner_across.show([pair], si, from_exp(k), par)

    def of_clip(value, c):
        return value.reshape(exp_n, clips, owned, value.shape[-1])[:, c].reshape(slots, value.shape[-1])

    def spread(value, c):
        value = value.reshape(exp_n, 1, owned, value.shape[-1])
        zero = jnp.zeros_like(value)
        parts = [value if k == c else zero for k in range(clips)]
        return jnp.concatenate(parts, axis=1).reshape(clips * slots, value.shape[-1])

    stat_across.arrived()
    columns.arrived()
    owners = [(g, q) for g in range(half) for q in range(2)]
    so = jnp.concatenate(
        [jnp.concatenate([so_ag[q, t, g] for t in range(seq_n)], axis=1) for g, q in owners], axis=0
    )
    stats = sa[...].reshape(slots, 128)
    for c in range(clips):
        mixing = qf[c]
        mixing_grad = of_clip(dot_nt(so, gout[c]), c)
        lm[c] = mixing * (mixing_grad - jnp.sum(mixing * mixing_grad, axis=0, keepdims=True))
        mass = stats[:, clips + c : clips + c + 1]
        dsp[c] = jnp.exp(lg[c] - stats[:, c : c + 1]) / mass
    across.arrived()
    inner_across.arrived()
    sig = sig_ag[...].reshape(exp_n * nr, width)
    inners = si[...].reshape(slots, 128)
    gr = 0.0
    for c in range(clips):
        dispatch_grad = of_clip(dot_nt(sig, tok[c]), c)
        lgrad = dsp[c] * (dispatch_grad - inners[:, c : c + 1]) + lm[c]
        lm[c] = lgrad
        gr = gr + dot(lgrad.astype(BF16), tok[c])

    out_rows = gr_o.shape[0]
    packed = gr_b.shape[2]
    pack = out_rows // packed
    whole = gr.T
    for t in range(seq_n):
        for g in range(half):
            for q in range(2):
                at = (t * exp_n + 2 * g + q) * out_rows
                parts = [whole[at + j * packed : at + (j + 1) * packed] for j in range(pack)]
                gr_a[q, t, g] = jnp.concatenate(parts, axis=1).astype(BF16)
    last = net.group(gr_p).start(gr_a.at[1 - par], gr_p, pair)
    both = jnp.concatenate([rt[...], sig], axis=0)

    def token_grad(c):
        left = jnp.concatenate([lm[c], spread(dsp[c], c)], axis=0)
        gt[c] = dot(left.T.astype(BF16), both).astype(BF16)

    last.arrived()
    gr_b[...] = (gr_a[par].astype(F32) + gr_p[...].astype(F32)).astype(BF16)
    last = net.group(gr_r)
    for k, (t, g) in enumerate(there):
        last.start(gr_b.at[t, g], gr_r.at[k], far_peers[k])
    for c in range(clips):
        mixed[c] = dot(spread(qf[c], c).T.astype(BF16), so).astype(BF16)
        token_grad(c)
    total = gr_b[s, h].astype(F32)
    last.arrived()
    for k in range(len(there)):
        total = total + gr_r[k].astype(F32)
    for j in range(pack):
        gr_o[j * packed : (j + 1) * packed] = total[:, j * slots : (j + 1) * slots]
    net.drain()
    assert len(net.groups) == groups_of(seq_n, exp_n)


def put_out(n, *refs):
    ins, outs, sem = refs[:n], refs[n : 2 * n], refs[2 * n]
    copies = []
    for src, dst in zip(ins, outs):
        copies.append(pltpu.make_async_copy(src, dst, sem.at[len(copies)]))
        copies[-1].start()
    for copy in copies:
        copy.wait()


def on_device(seq_n, exp_n, tokens, router, w_in, w_out, grad_out):
    clips, rows, width = tokens.shape
    slots = router.shape[1]
    half = exp_n // 2
    owned = slots // exp_n
    nr = clips * owned
    vmem = pl.BlockSpec(memory_space=pltpu.VMEM)
    hbm = pl.BlockSpec(memory_space=pltpu.HBM)
    anywhere = pl.BlockSpec(memory_space=pl.ANY)
    shape = jax.ShapeDtypeStruct
    out_rows = width // (seq_n * exp_n)
    pack = max(1, 128 // slots)
    tile = (out_rows // pack, slots * pack)
    piece = (nr, width)
    part = (nr, width // seq_n)
    stat = (owned, 128)
    n_groups = groups_of(seq_n, exp_n)
    outs = (
        shape(tokens.shape, BF16),
        shape(tokens.shape, BF16),
        shape(w_in.shape, BF16),
        shape(w_out.shape, BF16),
        shape((out_rows, slots), F32),
    )
    limit = VMEM_BYTES // 2
    results = pl.pallas_call(
        functools.partial(layer, seq_n, exp_n),
        out_shape=outs,
        in_specs=[hbm] * 5,
        out_specs=(vmem,) * 5,
        scratch_shapes=[
            pltpu.VMEM(tokens.shape, BF16),
            pltpu.VMEM(tokens.shape, BF16),
            pltpu.VMEM((slots, width), BF16),
            pltpu.VMEM(w_in.shape, BF16),
            pltpu.VMEM(w_out.shape, BF16),
            pltpu.VMEM((clips, slots, rows), F32),
            pltpu.VMEM((clips, slots, rows), F32),
            pltpu.VMEM((clips, slots, rows), F32),
            pltpu.VMEM((clips, slots, rows), F32),
            pltpu.VMEM((clips, slots, rows), BF16),
            pltpu.VMEM((clips, slots, rows), BF16),
            pltpu.VMEM((2, 2, half) + piece, BF16),
            pltpu.VMEM((2, half) + piece, BF16),
            pltpu.VMEM((half,) + piece, BF16),
            pltpu.VMEM((half - 1,) + piece, BF16),
            pltpu.VMEM((seq_n,) + piece, BF16),
            pltpu.VMEM((seq_n, half) + part, BF16),
            pltpu.VMEM((seq_n - 1, half) + part, BF16),
            pltpu.VMEM((half,) + part, BF16),
            pltpu.VMEM((half - 1,) + part, BF16),
            pltpu.VMEM((seq_n,) + part, BF16),
            pltpu.VMEM((seq_n,) + part, BF16),
            pltpu.VMEM((seq_n - 1,) + part, BF16),
            pltpu.VMEM((seq_n,) + piece, BF16),
            pltpu.VMEM((2, seq_n, half) + part, BF16),
            pltpu.VMEM((half, 2) + piece, BF16),
            pltpu.VMEM((2, half) + stat, F32),
            pltpu.VMEM((half,) + stat, F32),
            pltpu.VMEM((half,) + stat, F32),
            pltpu.VMEM((half - 1,) + stat, F32),
            pltpu.VMEM((seq_n,) + stat, F32),
            pltpu.VMEM((half, 2) + stat, F32),
            pltpu.VMEM((half, 2) + stat, F32),
            pltpu.VMEM((2, seq_n, half) + tile, BF16),
            pltpu.VMEM((seq_n, half) + tile, BF16),
            pltpu.VMEM((seq_n, half) + tile, BF16),
            pltpu.VMEM((seq_n * half - 1,) + tile, BF16),
            pltpu.SemaphoreType.DMA((2 * clips + 3,)),
            pltpu.SemaphoreType.DMA((n_groups,)),
            pltpu.SemaphoreType.DMA((n_groups,)),
        ],
        compiler_params=pltpu.CompilerParams(
            collective_id=0, has_side_effects=True, vmem_limit_bytes=limit
        ),
        name="layer",
    )(*[pltpu.with_memory_space_constraint(a, pltpu.HBM) for a in (tokens, router.T, grad_out, w_in, w_out)])
    mixed, grad_tokens, grad_w_in, grad_w_out, grad_router = pl.pallas_call(
        functools.partial(put_out, len(outs)),
        out_shape=outs,
        in_specs=[anywhere] * len(outs),
        out_specs=(hbm,) * len(outs),
        scratch_shapes=[pltpu.SemaphoreType.DMA((len(outs),))],
        compiler_params=pltpu.CompilerParams(vmem_limit_bytes=2**20),
        name="put_out",
    )(*results)
    return mixed, grad_tokens, grad_router, grad_w_in, grad_w_out


def solution(mesh):
    return jax.shard_map(
        functools.partial(on_device, mesh.shape["seq"], mesh.shape["exp"]),
        mesh=mesh,
        in_specs=(
            P(None, ("seq", "exp"), None),
            P(),
            P("exp", None, "seq"),
            P("exp", "seq", None),
            P(None, ("seq", "exp"), None),
        ),
        out_specs=(
            P(None, ("seq", "exp"), None),
            P(None, ("seq", "exp"), None),
            P(("seq", "exp"), None),
            P("exp", None, "seq"),
            P("exp", "seq", None),
        ),
        check_vma=False,
    )
```

```python
import functools

import jax
import jax.numpy as jnp
from jax import lax
from jax.experimental import pallas as pl
from jax.experimental.pallas import tpu as pltpu
from jax.sharding import PartitionSpec as P

MESH = pl.DeviceIdType.MESH
F32 = jnp.float32
BF16 = jnp.bfloat16
NT = (((1,), (1,)), ((), ()))
VMEM_BYTES = 67043328


def dot(a, b):
    return jnp.dot(a, b, preferred_element_type=F32)


def dot_nt(a, b):
    return lax.dot_general(a, b, NT, preferred_element_type=F32)


def place(seq_n, exp_n):
    s = lax.axis_index("seq")
    e = lax.axis_index("exp")
    half = exp_n // 2
    h, par = e // 2, e % 2
    pair = (s, h * 2 + (1 - par))
    seq_peers = [((s + k) % seq_n, e) for k in range(1, seq_n)]
    exp_peers = [(s, ((h + k) % half) * 2 + par) for k in range(1, half)]
    there = [((s + a) % seq_n, (h + b) % half) for a in range(seq_n) for b in range(half) if a or b]
    return s, h, par, pair, seq_peers, exp_peers, there


class Net:
    def __init__(self, send_sem, recv_sem):
        self.send_sem, self.recv_sem, self.groups = send_sem, recv_sem, []

    def group(self, whole):
        self.groups.append(whole)
        return Group(self, len(self.groups) - 1, whole)

    def drain(self):
        for i, whole in enumerate(self.groups):
            pltpu.make_async_copy(whole, whole, self.send_sem.at[i]).wait()


class Group:
    def __init__(self, net, index, whole):
        self.net, self.index, self.whole = net, index, whole

    def start(self, src, dst, peer):
        pltpu.make_async_remote_copy(
            src_ref=src,
            dst_ref=dst,
            send_sem=self.net.send_sem.at[self.index],
            recv_sem=self.net.recv_sem.at[self.index],
            device_id=peer,
            device_id_type=MESH,
        ).start()
        return self

    def show(self, peers, ref, *at):
        for peer in peers:
            self.start(ref.at[at], ref.at[at], peer)
        return self

    def arrived(self):
        pltpu.make_async_copy(self.whole, self.whole, self.net.recv_sem.at[self.index]).wait()


def groups_of(seq_n, exp_n):
    return 21 + (seq_n - 1) + (exp_n // 2 - 1)


def stat_tile(columns):
    shape = columns[0].shape[:-1] + (128,)
    lane = lax.broadcasted_iota(jnp.int32, shape, len(shape) - 1)
    tile = jnp.zeros(shape, F32)
    for i, column in enumerate(columns):
        tile = jnp.where(lane == i, column, tile)
    return tile


def by_clip(column, clips):
    owned = column.shape[-2] // clips
    return [column[..., c * owned : (c + 1) * owned, :] for c in range(clips)]


def split_stats(tile, clips):
    lanes = [tile[..., i : i + 1] for i in range(2 * clips)]
    axis = len(tile.shape) - 2
    return jnp.concatenate(lanes[:clips], axis=axis), jnp.concatenate(lanes[clips:], axis=axis)


def join(parts):
    peak = parts[0][0]
    for p, _ in parts[1:]:
        peak = jnp.maximum(peak, p)
    factors = [jnp.exp(p - peak) for p, _ in parts]
    mass = factors[0] * parts[0][1]
    for f, (_, m) in zip(factors[1:], parts[1:]):
        mass = mass + f * m
    return peak, mass, factors


def layer(
    seq_n, exp_n, tok_hbm, rt_hbm, gout_hbm, win_hbm, wout_hbm,
    mixed, gt, gwin, gwout, gr_o,
    tok, gout, rt, win, wout, tok_t, gout_t, win_t, wout_t, lg, qf, dsp, lm, xt, qt,
    buf_a, rcv_a, xb, xr, xg, gb, gbr, gc, gcr, gg, fe, fer, se, so_ag, sig_ag,
    st_a, st_p, st_b, st_z, st_c, sa, si,
    gr_a, gr_p, gr_b, gr_r,
    w_sem, send_sem, recv_sem,
):
    clips, rows, width = tok.shape
    slots = rt.shape[0]
    half = exp_n // 2
    owned = slots // exp_n
    nr = clips * owned
    dc = width // seq_n
    experts = win.shape[0]
    s, h, par, pair, seq_peers, exp_peers, there = place(seq_n, exp_n)
    far_peers = [(t, g * 2 + par) for t, g in there]

    load_rt = pltpu.make_async_copy(rt_hbm, rt, w_sem.at[0])
    load_tok = [pltpu.make_async_copy(tok_hbm.at[c], tok.at[c], w_sem.at[1 + c]) for c in range(clips)]
    load_gout = [
        pltpu.make_async_copy(gout_hbm.at[c], gout.at[c], w_sem.at[1 + clips + c]) for c in range(clips)
    ]
    load_in = pltpu.make_async_copy(win_hbm, win, w_sem.at[1 + 2 * clips])
    load_out = pltpu.make_async_copy(wout_hbm, wout, w_sem.at[2 + 2 * clips])
    load_rt.start()
    for load in load_tok + load_gout:
        load.start()
    barrier = pltpu.get_barrier_semaphore()
    for peer in [pair] + far_peers:
        pl.semaphore_signal(barrier, inc=1, device_id=peer, device_id_type=MESH)
    net = Net(send_sem, recv_sem)

    load_rt.wait()
    values, peaks, masses = [], [], []
    for c in range(clips):
        load_tok[c].wait()
        values.append(dot_nt(rt[...], tok[c]))
    for c, value in enumerate(values):
        lg[c] = value
        peak = jnp.max(value, axis=1, keepdims=True)
        p = jnp.exp(value - peak)
        peaks.append(peak.reshape(half, 2, owned, 1))
        masses.append(jnp.sum(p, axis=1, keepdims=True).reshape(half, 2, owned, 1))
        xt[c] = p.astype(BF16)
    for c, value in enumerate(values):
        q = jnp.exp(value - jnp.max(value, axis=0, keepdims=True))
        q = q / jnp.sum(q, axis=0, keepdims=True)
        qf[c] = q
        qt[c] = q.astype(BF16)
    tile = stat_tile(peaks + masses)
    for q in range(2):
        st_a[q] = tile[:, q]

    def lay_out(kind, values):
        for g in range(half):
            for q in range(2):
                at = (2 * g + q) * owned
                rows_ = [value[at : at + owned] for value in values]
                buf_a[kind, q, g] = jnp.concatenate(rows_, axis=0).astype(BF16)

    def pair_sum(kind, g, factors=None):
        mine = buf_a[kind, par, g].astype(F32)
        other = rcv_a[kind, g].astype(F32)
        if factors is not None:
            mine, other = mine * factors[0][g], other * factors[1][g]
        return (mine + other).astype(BF16)

    def spread_over(peers, at, ref, dst):
        group = net.group(dst)
        for k, peer in enumerate(peers):
            group.start(ref.at[at(k)], dst.at[k], peer)
        return group

    def show_seq(ref):
        return net.group(ref.at[pl.ds(0, seq_n - 1)]).show(seq_peers, ref, s)

    def exp_of(k):
        return (h + 1 + k) % half

    def seq_of(k):
        return (s + 1 + k) % seq_n

    def add_up(parts, factors=None):
        parts = [part.astype(F32) for part in parts]
        if factors is not None:
            parts = [part * f for part, f in zip(parts, factors)]
        total = parts[0]
        for part in parts[1:]:
            total = total + part
        return total

    lay_out(0, [dot(xt[c], tok[c]) for c in range(clips)])
    pl.semaphore_wait(barrier, 1 + len(far_peers))
    stat = net.group(st_p).start(st_a.at[1 - par], st_p, pair)
    inputs = net.group(rcv_a.at[0]).start(buf_a.at[0, 1 - par], rcv_a.at[0], pair)
    for load in load_gout:
        load.wait()
    lay_out(1, [dot(qt[c], gout[c]) for c in range(clips)])
    grads = net.group(rcv_a.at[1]).start(buf_a.at[1, 1 - par], rcv_a.at[1], pair)
    load_out.start()
    load_in.start()

    stat.arrived()
    peak, mass, fac = join([split_stats(st_a[par], clips), split_stats(st_p[...], clips)])
    st_b[...] = stat_tile(by_clip(peak, clips) + by_clip(mass, clips))
    stat = spread_over(exp_peers, exp_of, st_b, st_z)
    inputs.arrived()
    for g in range(half):
        xb[g] = pair_sum(0, g, fac)
    inputs = spread_over(exp_peers, exp_of, xb, xr)
    grads.arrived()
    for g in range(half):
        value = pair_sum(1, g)
        for t in range(seq_n):
            gb[t, g] = value[:, t * dc : (t + 1) * dc]
    grads = spread_over(seq_peers, seq_of, gb, gbr)
    for c in range(clips):
        tok_t[c] = tok[c].T
        gout_t[c] = gout[c].T
    stat.arrived()
    parts = [split_stats(st_b[h], clips)] + [split_stats(st_z[k], clips) for k in range(half - 1)]
    peak, mass, fac = join(parts)
    st_c[s] = stat_tile(by_clip(peak, clips) + by_clip(mass, clips))
    stat = show_seq(st_c)
    grads.arrived()
    for g in range(half):
        gc[g] = add_up([gb[s, g]] + [gbr[k, g] for k in range(seq_n - 1)]).astype(BF16)
    grads = spread_over(exp_peers, exp_of, gc, gcr)
    inputs.arrived()
    xg[s] = add_up([xb[h]] + [xr[k] for k in range(half - 1)], fac).astype(BF16)
    inputs = show_seq(xg)
    load_out.wait()
    load_in.wait()
    for e in range(experts):
        wout_t[e] = wout[e].T
    for e in range(experts // 2):
        win_t[e] = win[e].T
    stat.arrived()
    peak, mass, fac = join([split_stats(st_c[t], clips) for t in range(seq_n)])
    fac = [f / mass for f in fac]
    sa[h, par] = stat_tile(by_clip(peak, clips) + by_clip(mass, clips))
    stat_along = net.group(sa.at[pl.ds(0, half - 1), 0]).show(exp_peers, sa, h, par)
    stat_across = net.group(sa.at[pl.ds(0, half), 0]).show([pair], sa, h, par)
    grads.arrived()
    gg[s] = add_up([gc[h]] + [gcr[k] for k in range(half - 1)]).astype(BF16)
    grads = show_seq(gg)

    row = lax.broadcasted_iota(jnp.int32, (nr, 1), 0)
    expert_of = (row % owned) // (owned // experts)
    mask = [(expert_of == e).astype(F32) for e in range(experts)]
    inputs.arrived()
    x_rows = add_up([xg[t] for t in range(seq_n)], fac)
    pre = 0.0
    for e in range(experts):
        pre = pre + dot((x_rows * mask[e]).astype(BF16), win[e])
    hidden, back = jax.vjp(jax.nn.gelu, pre)
    out_part = 0.0
    for e in range(experts):
        out_part = out_part + dot((hidden * mask[e]).astype(BF16), wout[e])
    for t in range(seq_n):
        fe[t] = out_part[:, t * dc : (t + 1) * dc].astype(BF16)
    forward = spread_over(seq_peers, seq_of, fe, fer)
    for e in range(experts // 2, experts):
        win_t[e] = win[e].T
    grads.arrived()
    g_rows = jnp.concatenate([gg[t] for t in range(seq_n)], axis=1)
    hidden_grad = 0.0
    for e in range(experts):
        hidden_grad = hidden_grad + dot(g_rows, wout_t[e]) * mask[e]
    pre_grad = back(hidden_grad)[0]
    in_part = 0.0
    for e in range(experts):
        in_part = in_part + dot((pre_grad * mask[e]).astype(BF16), win_t[e])
    se[s] = in_part.astype(BF16)
    backward = show_seq(se)

    def from_exp(k):
        return (h + half - 1 - k) % half

    def weight_grad(out, e, left, right):
        out[e] = dot((left * mask[e]).T.astype(BF16), right).astype(BF16)

    forward.arrived()
    so_ag[par, s, h] = add_up([fe[s]] + [fer[k] for k in range(seq_n - 1)]).astype(BF16)
    forward = net.group(so_ag.at[0, 0, pl.ds(0, half - 1)]).show(exp_peers, so_ag, par, s, h)
    stat_along.arrived()
    for k in range(half - 1):
        stat_across.show([pair], sa, from_exp(k), par)
    for e in range(experts):
        weight_grad(gwout, e, hidden, g_rows)
    pg = pre_grad.astype(BF16)
    weight_grad(gwin, 0, x_rows, pg)
    forward.arrived()
    forward = [net.group(so_ag.at[0, 0]).show([peer], so_ag, par, s) for peer in seq_peers]
    columns = net.group(so_ag.at[0]).show([pair], so_ag, par, s)
    backward.arrived()
    piece = add_up([se[t] for t in range(seq_n)]).astype(BF16)
    sig_ag[h, par] = piece
    inner = jnp.sum(piece.astype(F32) * x_rows, axis=1, keepdims=True)
    si[h, par] = stat_tile(by_clip(inner, clips))
    along = [net.group(sig_ag.at[0, 0]).show([peer], sig_ag, h, par) for peer in exp_peers]
    inner_along = net.group(si.at[pl.ds(0, half - 1), 0]).show(exp_peers, si, h, par)
    across = net.group(sig_ag.at[pl.ds(0, half), 0]).show([pair], sig_ag, h, par)
    inner_across = net.group(si.at[pl.ds(0, half), 0]).show([pair], si, h, par)
    for e in range(1, experts):
        weight_grad(gwin, e, x_rows, pg)
    for k in range(seq_n - 1):
        forward[k].arrived()
        columns.show([pair], so_ag, par, (s + seq_n - 1 - k) % seq_n)
    for k in range(half - 1):
        along[k].arrived()
        across.show([pair], sig_ag, from_exp(k), par)
    inner_along.arrived()
    for k in range(half - 1):
        inner_across.show([pair], si, from_exp(k), par)

    def of_clip(value, c):
        return value.reshape(exp_n, clips, owned, value.shape[-1])[:, c].reshape(slots, value.shape[-1])

    def spread(value, c):
        value = value.reshape(exp_n, 1, owned, value.shape[-1])
        zero = jnp.zeros_like(value)
        parts = [value if k == c else zero for k in range(clips)]
        return jnp.concatenate(parts, axis=1).reshape(clips * slots, value.shape[-1])

    stat_across.arrived()
    columns.arrived()
    owners = [(g, q) for g in range(half) for q in range(2)]
    so = jnp.concatenate(
        [jnp.concatenate([so_ag[q, t, g] for t in range(seq_n)], axis=1) for g, q in owners], axis=0
    )
    stats = sa[...].reshape(slots, 128)
    for c in range(clips):
        mixing = qf[c]
        mixing_grad = of_clip(dot(so, gout_t[c]), c)
        lm[c] = mixing * (mixing_grad - jnp.sum(mixing * mixing_grad, axis=0, keepdims=True))
        mass = stats[:, clips + c : clips + c + 1]
        dsp[c] = jnp.exp(lg[c] - stats[:, c : c + 1]) / mass
    across.arrived()
    inner_across.arrived()
    sig = sig_ag[...].reshape(exp_n * nr, width)
    inners = si[...].reshape(slots, 128)
    gr = 0.0
    for c in range(clips):
        dispatch_grad = of_clip(dot(sig, tok_t[c]), c)
        lgrad = dsp[c] * (dispatch_grad - inners[:, c : c + 1]) + lm[c]
        lm[c] = lgrad
        gr = gr + dot(lgrad.astype(BF16), tok[c])

    out_rows = gr_o.shape[0]
    packed = gr_b.shape[2]
    pack = out_rows // packed
    whole = gr.T
    for t in range(seq_n):
        for g in range(half):
            for q in range(2):
                at = (t * exp_n + 2 * g + q) * out_rows
                parts = [whole[at + j * packed : at + (j + 1) * packed] for j in range(pack)]
                gr_a[q, t, g] = jnp.concatenate(parts, axis=1).astype(BF16)
    last = net.group(gr_p).start(gr_a.at[1 - par], gr_p, pair)
    both = jnp.concatenate([rt[...], sig], axis=0)

    def token_grad(c):
        left = jnp.concatenate([lm[c], spread(dsp[c], c)], axis=0)
        gt[c] = dot(left.T.astype(BF16), both).astype(BF16)

    last.arrived()
    gr_b[...] = (gr_a[par].astype(F32) + gr_p[...].astype(F32)).astype(BF16)
    last = net.group(gr_r)
    for k, (t, g) in enumerate(there):
        last.start(gr_b.at[t, g], gr_r.at[k], far_peers[k])
    for c in range(clips):
        mixed[c] = dot(spread(qf[c], c).T.astype(BF16), so).astype(BF16)
        token_grad(c)
    total = gr_b[s, h].astype(F32)
    last.arrived()
    for k in range(len(there)):
        total = total + gr_r[k].astype(F32)
    for j in range(pack):
        gr_o[j * packed : (j + 1) * packed] = total[:, j * slots : (j + 1) * slots]
    net.drain()
    assert len(net.groups) == groups_of(seq_n, exp_n)


def put_out(n, *refs):
    ins, outs, sem = refs[:n], refs[n : 2 * n], refs[2 * n]
    copies = []
    for src, dst in zip(ins, outs):
        copies.append(pltpu.make_async_copy(src, dst, sem.at[len(copies)]))
        copies[-1].start()
    for copy in copies:
        copy.wait()


def on_device(seq_n, exp_n, tokens, router, w_in, w_out, grad_out):
    clips, rows, width = tokens.shape
    slots = router.shape[1]
    experts, _, ff = w_in.shape
    half = exp_n // 2
    owned = slots // exp_n
    nr = clips * owned
    vmem = pl.BlockSpec(memory_space=pltpu.VMEM)
    hbm = pl.BlockSpec(memory_space=pltpu.HBM)
    anywhere = pl.BlockSpec(memory_space=pl.ANY)
    shape = jax.ShapeDtypeStruct
    out_rows = width // (seq_n * exp_n)
    pack = max(1, 128 // slots)
    tile = (out_rows // pack, slots * pack)
    piece = (nr, width)
    part = (nr, width // seq_n)
    stat = (owned, 128)
    n_groups = groups_of(seq_n, exp_n)
    outs = (
        shape(tokens.shape, BF16),
        shape(tokens.shape, BF16),
        shape(w_in.shape, BF16),
        shape(w_out.shape, BF16),
        shape((out_rows, slots), F32),
    )
    limit = VMEM_BYTES // 16 * 9
    results = pl.pallas_call(
        functools.partial(layer, seq_n, exp_n),
        out_shape=outs,
        in_specs=[hbm] * 5,
        out_specs=(vmem,) * 5,
        scratch_shapes=[
            pltpu.VMEM(tokens.shape, BF16),
            pltpu.VMEM(tokens.shape, BF16),
            pltpu.VMEM((slots, width), BF16),
            pltpu.VMEM(w_in.shape, BF16),
            pltpu.VMEM(w_out.shape, BF16),
            pltpu.VMEM((clips, width, rows), BF16),
            pltpu.VMEM((clips, width, rows), BF16),
            pltpu.VMEM((experts, ff, width), BF16),
            pltpu.VMEM((experts, width, ff), BF16),
            pltpu.VMEM((clips, slots, rows), F32),
            pltpu.VMEM((clips, slots, rows), F32),
            pltpu.VMEM((clips, slots, rows), F32),
            pltpu.VMEM((clips, slots, rows), F32),
            pltpu.VMEM((clips, slots, rows), BF16),
            pltpu.VMEM((clips, slots, rows), BF16),
            pltpu.VMEM((2, 2, half) + piece, BF16),
            pltpu.VMEM((2, half) + piece, BF16),
            pltpu.VMEM((half,) + piece, BF16),
            pltpu.VMEM((half - 1,) + piece, BF16),
            pltpu.VMEM((seq_n,) + piece, BF16),
            pltpu.VMEM((seq_n, half) + part, BF16),
            pltpu.VMEM((seq_n - 1, half) + part, BF16),
            pltpu.VMEM((half,) + part, BF16),
            pltpu.VMEM((half - 1,) + part, BF16),
            pltpu.VMEM((seq_n,) + part, BF16),
            pltpu.VMEM((seq_n,) + part, BF16),
            pltpu.VMEM((seq_n - 1,) + part, BF16),
            pltpu.VMEM((seq_n,) + piece, BF16),
            pltpu.VMEM((2, seq_n, half) + part, BF16),
            pltpu.VMEM((half, 2) + piece, BF16),
            pltpu.VMEM((2, half) + stat, F32),
            pltpu.VMEM((half,) + stat, F32),
            pltpu.VMEM((half,) + stat, F32),
            pltpu.VMEM((half - 1,) + stat, F32),
            pltpu.VMEM((seq_n,) + stat, F32),
            pltpu.VMEM((half, 2) + stat, F32),
            pltpu.VMEM((half, 2) + stat, F32),
            pltpu.VMEM((2, seq_n, half) + tile, BF16),
            pltpu.VMEM((seq_n, half) + tile, BF16),
            pltpu.VMEM((seq_n, half) + tile, BF16),
            pltpu.VMEM((seq_n * half - 1,) + tile, BF16),
            pltpu.SemaphoreType.DMA((2 * clips + 3,)),
            pltpu.SemaphoreType.DMA((n_groups,)),
            pltpu.SemaphoreType.DMA((n_groups,)),
        ],
        compiler_params=pltpu.CompilerParams(
            collective_id=0, has_side_effects=True, vmem_limit_bytes=limit
        ),
        name="layer",
    )(*[pltpu.with_memory_space_constraint(a, pltpu.HBM) for a in (tokens, router.T, grad_out, w_in, w_out)])
    mixed, grad_tokens, grad_w_in, grad_w_out, grad_router = pl.pallas_call(
        functools.partial(put_out, len(outs)),
        out_shape=outs,
        in_specs=[anywhere] * len(outs),
        out_specs=(hbm,) * len(outs),
        scratch_shapes=[pltpu.SemaphoreType.DMA((len(outs),))],
        compiler_params=pltpu.CompilerParams(vmem_limit_bytes=2**20),
        name="put_out",
    )(*results)
    return mixed, grad_tokens, grad_router, grad_w_in, grad_w_out


def solution(mesh):
    return jax.shard_map(
        functools.partial(on_device, mesh.shape["seq"], mesh.shape["exp"]),
        mesh=mesh,
        in_specs=(
            P(None, ("seq", "exp"), None),
            P(),
            P("exp", None, "seq"),
            P("exp", "seq", None),
            P(None, ("seq", "exp"), None),
        ),
        out_specs=(
            P(None, ("seq", "exp"), None),
            P(None, ("seq", "exp"), None),
            P(("seq", "exp"), None),
            P("exp", None, "seq"),
            P("exp", "seq", None),
        ),
        check_vma=False,
    )
```

```python
import functools

import jax
import jax.numpy as jnp
from jax import lax
from jax.experimental import pallas as pl
from jax.experimental.pallas import tpu as pltpu
from jax.sharding import PartitionSpec as P

MESH = pl.DeviceIdType.MESH
F32 = jnp.float32
BF16 = jnp.bfloat16
NT = (((1,), (1,)), ((), ()))
VMEM_BYTES = 67043328


def dot(a, b):
    return jnp.dot(a, b, preferred_element_type=F32)


def dot_nt(a, b):
    return lax.dot_general(a, b, NT, preferred_element_type=F32)


def place(seq_n, exp_n):
    s = lax.axis_index("seq")
    e = lax.axis_index("exp")
    half = exp_n // 2
    h, par = e // 2, e % 2
    pair = (s, h * 2 + (1 - par))
    seq_peers = [((s + k) % seq_n, e) for k in range(1, seq_n)]
    exp_peers = [(s, ((h + k) % half) * 2 + par) for k in range(1, half)]
    ways = [(a, b) for a in range(seq_n) for b in range(half) if a or b]
    there = [((s + a) % seq_n, (h + b) % half) for a, b in ways]
    return s, h, par, pair, seq_peers, exp_peers, ways, there


class Net:
    def __init__(self, send_sem, recv_sem):
        self.send_sem, self.recv_sem, self.groups = send_sem, recv_sem, []

    def group(self, whole):
        self.groups.append(whole)
        return Group(self, len(self.groups) - 1, whole)

    def drain(self):
        for i, whole in enumerate(self.groups):
            pltpu.make_async_copy(whole, whole, self.send_sem.at[i]).wait()


class Group:
    def __init__(self, net, index, whole):
        self.net, self.index, self.whole = net, index, whole

    def start(self, src, dst, peer):
        pltpu.make_async_remote_copy(
            src_ref=src,
            dst_ref=dst,
            send_sem=self.net.send_sem.at[self.index],
            recv_sem=self.net.recv_sem.at[self.index],
            device_id=peer,
            device_id_type=MESH,
        ).start()
        return self

    def show(self, peers, ref, *at):
        for peer in peers:
            self.start(ref.at[at], ref.at[at], peer)
        return self

    def arrived(self):
        pltpu.make_async_copy(self.whole, self.whole, self.net.recv_sem.at[self.index]).wait()


def groups_of(seq_n, exp_n):
    return 21 + (seq_n - 1) + (exp_n // 2 - 1)


def stat_tile(columns):
    shape = columns[0].shape[:-1] + (128,)
    lane = lax.broadcasted_iota(jnp.int32, shape, len(shape) - 1)
    tile = jnp.zeros(shape, F32)
    for i, column in enumerate(columns):
        tile = jnp.where(lane == i, column, tile)
    return tile


def by_clip(column, clips):
    owned = column.shape[-2] // clips
    return [column[..., c * owned : (c + 1) * owned, :] for c in range(clips)]


def split_stats(tile, clips):
    lanes = [tile[..., i : i + 1] for i in range(2 * clips)]
    axis = len(tile.shape) - 2
    return jnp.concatenate(lanes[:clips], axis=axis), jnp.concatenate(lanes[clips:], axis=axis)


def join(parts):
    peak = parts[0][0]
    for p, _ in parts[1:]:
        peak = jnp.maximum(peak, p)
    factors = [jnp.exp(p - peak) for p, _ in parts]
    mass = factors[0] * parts[0][1]
    for f, (_, m) in zip(factors[1:], parts[1:]):
        mass = mass + f * m
    return peak, mass, factors


def layer(
    seq_n, exp_n, tok_hbm, rt_hbm, gout_hbm, win_hbm, wout_hbm,
    mixed, gt, gwin, gwout, gr_o,
    tok, gout, rt, win, wout, tok_t, gout_t, win_t, wout_t, lg, qf, dsp, lm, xt, qt,
    buf_a, rcv_a, xb, xr, xg, gb, gbr, gc, gcr, gg, fe, fer, se, so_ag, sig_ag,
    st_a, st_p, st_b, st_z, st_c, sa, si,
    gr_a, gr_p, gr_b, gr_r,
    w_sem, send_sem, recv_sem,
):
    clips, rows, width = tok.shape
    slots = rt.shape[0]
    half = exp_n // 2
    owned = slots // exp_n
    nr = clips * owned
    dc = width // seq_n
    experts = win.shape[0]
    s, h, par, pair, seq_peers, exp_peers, ways, there = place(seq_n, exp_n)
    far_peers = [(t, g * 2 + par) for t, g in there]

    load_rt = pltpu.make_async_copy(rt_hbm, rt, w_sem.at[0])
    load_tok = [
        pltpu.make_async_copy(tok_hbm.at[c], tok.at[c], w_sem.at[3 + clips + c]) for c in range(clips)
    ]
    load_gout = [
        pltpu.make_async_copy(gout_hbm.at[c], gout.at[c], w_sem.at[1 + c]) for c in range(clips)
    ]
    load_in = pltpu.make_async_copy(win_hbm, win, w_sem.at[1 + clips])
    load_out = pltpu.make_async_copy(wout_hbm, wout, w_sem.at[2 + clips])
    load_rt.start()
    for load in load_tok + load_gout:
        load.start()
    barrier = pltpu.get_barrier_semaphore()
    for peer in [pair] + far_peers:
        pl.semaphore_signal(barrier, inc=1, device_id=peer, device_id_type=MESH)
    net = Net(send_sem, recv_sem)

    load_rt.wait()
    values, peaks, masses = [], [], []
    for c in range(clips):
        load_tok[c].wait()
        values.append(dot_nt(rt[...], tok[c]))
    for c, value in enumerate(values):
        lg[c] = value
        peak = jnp.max(value, axis=1, keepdims=True)
        p = jnp.exp(value - peak)
        peaks.append(peak.reshape(half, 2, owned, 1))
        masses.append(jnp.sum(p, axis=1, keepdims=True).reshape(half, 2, owned, 1))
        xt[c] = p.astype(BF16)
    for c, value in enumerate(values):
        q = jnp.exp(value - jnp.max(value, axis=0, keepdims=True))
        q = q / jnp.sum(q, axis=0, keepdims=True)
        qf[c] = q
        qt[c] = q.astype(BF16)
    tile = stat_tile(peaks + masses)
    for q in range(2):
        st_a[q] = tile[:, q]

    def lay_out(kind, values):
        for g in range(half):
            for q in range(2):
                at = (2 * g + q) * owned
                rows_ = [value[at : at + owned] for value in values]
                buf_a[kind, q, g] = jnp.concatenate(rows_, axis=0).astype(BF16)

    def pair_sum(kind, g, factors=None):
        mine = buf_a[kind, par, g].astype(F32)
        other = rcv_a[kind, g].astype(F32)
        if factors is not None:
            mine, other = mine * factors[0][g], other * factors[1][g]
        return (mine + other).astype(BF16)

    def spread_over(peers, at, ref, dst):
        group = net.group(dst)
        for k, peer in enumerate(peers):
            group.start(ref.at[at(k)], dst.at[k], peer)
        return group

    def show_seq(ref):
        return net.group(ref.at[pl.ds(0, seq_n - 1)]).show(seq_peers, ref, s)

    def exp_of(k):
        return (h + 1 + k) % half

    def seq_of(k):
        return (s + 1 + k) % seq_n

    def add_up(parts, factors=None):
        parts = [part.astype(F32) for part in parts]
        if factors is not None:
            parts = [part * f for part, f in zip(parts, factors)]
        total = parts[0]
        for part in parts[1:]:
            total = total + part
        return total

    lay_out(0, [dot(xt[c], tok[c]) for c in range(clips)])
    pl.semaphore_wait(barrier, 1 + len(far_peers))
    stat = net.group(st_p).start(st_a.at[1 - par], st_p, pair)
    inputs = net.group(rcv_a.at[0]).start(buf_a.at[0, 1 - par], rcv_a.at[0], pair)
    for load in load_gout:
        load.wait()
    lay_out(1, [dot(qt[c], gout[c]) for c in range(clips)])
    grads = net.group(rcv_a.at[1]).start(buf_a.at[1, 1 - par], rcv_a.at[1], pair)
    load_out.start()
    load_in.start()

    stat.arrived()
    peak, mass, fac = join([split_stats(st_a[par], clips), split_stats(st_p[...], clips)])
    st_b[...] = stat_tile(by_clip(peak, clips) + by_clip(mass, clips))
    stat = spread_over(exp_peers, exp_of, st_b, st_z)
    inputs.arrived()
    for g in range(half):
        xb[g] = pair_sum(0, g, fac)
    inputs = spread_over(exp_peers, exp_of, xb, xr)
    grads.arrived()
    for g in range(half):
        value = pair_sum(1, g)
        for t in range(seq_n):
            gb[t, g] = value[:, t * dc : (t + 1) * dc]
    grads = spread_over(seq_peers, seq_of, gb, gbr)
    for c in range(clips):
        tok_t[c] = tok[c].T
        gout_t[c] = gout[c].T
    stat.arrived()
    parts = [split_stats(st_b[h], clips)] + [split_stats(st_z[k], clips) for k in range(half - 1)]
    peak, mass, fac = join(parts)
    st_c[s] = stat_tile(by_clip(peak, clips) + by_clip(mass, clips))
    stat = show_seq(st_c)
    grads.arrived()
    for g in range(half):
        gc[g] = add_up([gb[s, g]] + [gbr[k, g] for k in range(seq_n - 1)]).astype(BF16)
    grads = spread_over(exp_peers, exp_of, gc, gcr)
    inputs.arrived()
    xg[s] = add_up([xb[h]] + [xr[k] for k in range(half - 1)], fac).astype(BF16)
    inputs = show_seq(xg)
    load_out.wait()
    load_in.wait()
    for e in range(experts):
        wout_t[e] = wout[e].T
    for e in range(experts // 2):
        win_t[e] = win[e].T
    stat.arrived()
    peak, mass, fac = join([split_stats(st_c[t], clips) for t in range(seq_n)])
    fac = [f / mass for f in fac]
    sa[h, par] = stat_tile(by_clip(peak, clips) + by_clip(mass, clips))
    stat_along = net.group(sa.at[pl.ds(0, half - 1), 0]).show(exp_peers, sa, h, par)
    stat_across = net.group(sa.at[pl.ds(0, half), 0]).show([pair], sa, h, par)
    grads.arrived()
    gg[s] = add_up([gc[h]] + [gcr[k] for k in range(half - 1)]).astype(BF16)
    grads = show_seq(gg)
    for e in range(experts // 2, experts):
        win_t[e] = win[e].T

    row = lax.broadcasted_iota(jnp.int32, (nr, 1), 0)
    expert_of = (row % owned) // (owned // experts)
    mask = [(expert_of == e).astype(F32) for e in range(experts)]
    inputs.arrived()
    x_rows = add_up([xg[t] for t in range(seq_n)], fac)
    pre = 0.0
    for e in range(experts):
        pre = pre + dot((x_rows * mask[e]).astype(BF16), win[e])
    hidden, back = jax.vjp(jax.nn.gelu, pre)
    out_part = 0.0
    for e in range(experts):
        out_part = out_part + dot((hidden * mask[e]).astype(BF16), wout[e])
    for t in range(seq_n):
        fe[t] = out_part[:, t * dc : (t + 1) * dc].astype(BF16)
    forward = spread_over(seq_peers, seq_of, fe, fer)
    grads.arrived()
    g_rows = jnp.concatenate([gg[t] for t in range(seq_n)], axis=1)
    hidden_grad = 0.0
    for e in range(experts):
        hidden_grad = hidden_grad + dot(g_rows, wout_t[e]) * mask[e]
    pre_grad = back(hidden_grad)[0]
    in_part = 0.0
    for e in range(experts):
        in_part = in_part + dot((pre_grad * mask[e]).astype(BF16), win_t[e])
    se[s] = in_part.astype(BF16)
    backward = show_seq(se)

    def from_exp(k):
        return (h + half - 1 - k) % half

    def weight_grad(out, e, left, right):
        out[e] = dot((left * mask[e]).T.astype(BF16), right).astype(BF16)

    weight_grad(gwout, 0, hidden, g_rows)
    forward.arrived()
    so_ag[par, s, h] = add_up([fe[s]] + [fer[k] for k in range(seq_n - 1)]).astype(BF16)
    forward = []
    for a in range(seq_n):
        here = [peer for way, peer in zip(ways, far_peers) if way[0] == a]
        group = net.group(so_ag.at[0, 0, pl.ds(0, len(here))])
        group.show(here, so_ag, par, s, h)
        forward.append(group)
    columns = net.group(so_ag.at[0])
    stat_along.arrived()
    for k in range(half - 1):
        stat_across.show([pair], sa, from_exp(k), par)
    for e in range(1, experts):
        weight_grad(gwout, e, hidden, g_rows)
    pg = pre_grad.astype(BF16)
    backward.arrived()
    piece = add_up([se[t] for t in range(seq_n)]).astype(BF16)
    sig_ag[h, par] = piece
    inner = jnp.sum(piece.astype(F32) * x_rows, axis=1, keepdims=True)
    si[h, par] = stat_tile(by_clip(inner, clips))
    inner_along = net.group(si.at[pl.ds(0, half - 1), 0]).show(exp_peers, si, h, par)
    along = [net.group(sig_ag.at[0, 0]).show([peer], sig_ag, h, par) for peer in exp_peers]
    inner_across = net.group(si.at[pl.ds(0, half), 0]).show([pair], si, h, par)
    across = net.group(sig_ag.at[pl.ds(0, half), 0]).show([pair], sig_ag, h, par)
    for e in range(experts):
        weight_grad(gwin, e, x_rows, pg)
    for a in range(seq_n):
        forward[a].arrived()
        columns.show([pair], so_ag, par, (s + seq_n - a) % seq_n)
    inner_along.arrived()
    for k in range(half - 1):
        inner_across.show([pair], si, from_exp(k), par)
    for k in range(half - 1):
        along[k].arrived()
        across.show([pair], sig_ag, from_exp(k), par)

    def of_clip(value, c):
        return value.reshape(exp_n, clips, owned, value.shape[-1])[:, c].reshape(slots, value.shape[-1])

    def spread(value, c):
        value = value.reshape(exp_n, 1, owned, value.shape[-1])
        zero = jnp.zeros_like(value)
        parts = [value if k == c else zero for k in range(clips)]
        return jnp.concatenate(parts, axis=1).reshape(clips * slots, value.shape[-1])

    stat_across.arrived()
    columns.arrived()
    owners = [(g, q) for g in range(half) for q in range(2)]
    so = jnp.concatenate(
        [jnp.concatenate([so_ag[q, t, g] for t in range(seq_n)], axis=1) for g, q in owners], axis=0
    )
    stats = sa[...].reshape(slots, 128)
    for c in range(clips):
        mixing = qf[c]
        mixing_grad = of_clip(dot(so, gout_t[c]), c)
        lm[c] = mixing * (mixing_grad - jnp.sum(mixing * mixing_grad, axis=0, keepdims=True))
        mass = stats[:, clips + c : clips + c + 1]
        dsp[c] = jnp.exp(lg[c] - stats[:, c : c + 1]) / mass
    across.arrived()
    inner_across.arrived()
    sig = sig_ag[...].reshape(exp_n * nr, width)
    inners = si[...].reshape(slots, 128)
    gr = 0.0
    for c in range(clips):
        dispatch_grad = of_clip(dot(sig, tok_t[c]), c)
        lgrad = dsp[c] * (dispatch_grad - inners[:, c : c + 1]) + lm[c]
        lm[c] = lgrad
        gr = gr + dot(lgrad.astype(BF16), tok[c])

    out_rows = gr_o.shape[0]
    packed = gr_b.shape[2]
    pack = out_rows // packed
    whole = gr.T
    for t in range(seq_n):
        for g in range(half):
            for q in range(2):
                at = (t * exp_n + 2 * g + q) * out_rows
                parts = [whole[at + j * packed : at + (j + 1) * packed] for j in range(pack)]
                gr_a[q, t, g] = jnp.concatenate(parts, axis=1).astype(BF16)
    last = net.group(gr_p).start(gr_a.at[1 - par], gr_p, pair)
    both = jnp.concatenate([rt[...], sig], axis=0)

    def token_grad(c):
        left = jnp.concatenate([lm[c], spread(dsp[c], c)], axis=0)
        gt[c] = dot(left.T.astype(BF16), both).astype(BF16)

    last.arrived()
    gr_b[...] = (gr_a[par].astype(F32) + gr_p[...].astype(F32)).astype(BF16)
    last = net.group(gr_r)
    for k, (t, g) in enumerate(there):
        last.start(gr_b.at[t, g], gr_r.at[k], far_peers[k])
    for c in range(clips):
        mixed[c] = dot(spread(qf[c], c).T.astype(BF16), so).astype(BF16)
        token_grad(c)
    total = gr_b[s, h].astype(F32)
    last.arrived()
    for k in range(len(there)):
        total = total + gr_r[k].astype(F32)
    for j in range(pack):
        gr_o[j * packed : (j + 1) * packed] = total[:, j * slots : (j + 1) * slots]
    net.drain()
    assert len(net.groups) == groups_of(seq_n, exp_n)


def put_out(n, *refs):
    ins, outs, sem = refs[:n], refs[n : 2 * n], refs[2 * n]
    copies = []
    for src, dst in zip(ins, outs):
        copies.append(pltpu.make_async_copy(src, dst, sem.at[len(copies)]))
        copies[-1].start()
    for copy in copies:
        copy.wait()


def on_device(seq_n, exp_n, tokens, router, w_in, w_out, grad_out):
    clips, rows, width = tokens.shape
    slots = router.shape[1]
    experts, _, ff = w_in.shape
    half = exp_n // 2
    owned = slots // exp_n
    nr = clips * owned
    vmem = pl.BlockSpec(memory_space=pltpu.VMEM)
    hbm = pl.BlockSpec(memory_space=pltpu.HBM)
    anywhere = pl.BlockSpec(memory_space=pl.ANY)
    shape = jax.ShapeDtypeStruct
    out_rows = width // (seq_n * exp_n)
    pack = max(1, 128 // slots)
    tile = (out_rows // pack, slots * pack)
    piece = (nr, width)
    part = (nr, width // seq_n)
    stat = (owned, 128)
    n_groups = groups_of(seq_n, exp_n)
    outs = (
        shape(tokens.shape, BF16),
        shape(tokens.shape, BF16),
        shape(w_in.shape, BF16),
        shape(w_out.shape, BF16),
        shape((out_rows, slots), F32),
    )
    limit = VMEM_BYTES // 16 * 9
    results = pl.pallas_call(
        functools.partial(layer, seq_n, exp_n),
        out_shape=outs,
        in_specs=[hbm] * 5,
        out_specs=(vmem,) * 5,
        scratch_shapes=[
            pltpu.VMEM(tokens.shape, BF16),
            pltpu.VMEM(tokens.shape, BF16),
            pltpu.VMEM((slots, width), BF16),
            pltpu.VMEM(w_in.shape, BF16),
            pltpu.VMEM(w_out.shape, BF16),
            pltpu.VMEM((clips, width, rows), BF16),
            pltpu.VMEM((clips, width, rows), BF16),
            pltpu.VMEM((experts, ff, width), BF16),
            pltpu.VMEM((experts, width, ff), BF16),
            pltpu.VMEM((clips, slots, rows), F32),
            pltpu.VMEM((clips, slots, rows), F32),
            pltpu.VMEM((clips, slots, rows), F32),
            pltpu.VMEM((clips, slots, rows), F32),
            pltpu.VMEM((clips, slots, rows), BF16),
            pltpu.VMEM((clips, slots, rows), BF16),
            pltpu.VMEM((2, 2, half) + piece, BF16),
            pltpu.VMEM((2, half) + piece, BF16),
            pltpu.VMEM((half,) + piece, BF16),
            pltpu.VMEM((half - 1,) + piece, BF16),
            pltpu.VMEM((seq_n,) + piece, BF16),
            pltpu.VMEM((seq_n, half) + part, BF16),
            pltpu.VMEM((seq_n - 1, half) + part, BF16),
            pltpu.VMEM((half,) + part, BF16),
            pltpu.VMEM((half - 1,) + part, BF16),
            pltpu.VMEM((seq_n,) + part, BF16),
            pltpu.VMEM((seq_n,) + part, BF16),
            pltpu.VMEM((seq_n - 1,) + part, BF16),
            pltpu.VMEM((seq_n,) + piece, BF16),
            pltpu.VMEM((2, seq_n, half) + part, BF16),
            pltpu.VMEM((half, 2) + piece, BF16),
            pltpu.VMEM((2, half) + stat, F32),
            pltpu.VMEM((half,) + stat, F32),
            pltpu.VMEM((half,) + stat, F32),
            pltpu.VMEM((half - 1,) + stat, F32),
            pltpu.VMEM((seq_n,) + stat, F32),
            pltpu.VMEM((half, 2) + stat, F32),
            pltpu.VMEM((half, 2) + stat, F32),
            pltpu.VMEM((2, seq_n, half) + tile, BF16),
            pltpu.VMEM((seq_n, half) + tile, BF16),
            pltpu.VMEM((seq_n, half) + tile, BF16),
            pltpu.VMEM((seq_n * half - 1,) + tile, BF16),
            pltpu.SemaphoreType.DMA((2 * clips + 3,)),
            pltpu.SemaphoreType.DMA((n_groups,)),
            pltpu.SemaphoreType.DMA((n_groups,)),
        ],
        compiler_params=pltpu.CompilerParams(
            collective_id=0, has_side_effects=True, vmem_limit_bytes=limit
        ),
        name="layer",
    )(*[pltpu.with_memory_space_constraint(a, pltpu.HBM) for a in (tokens, router.T, grad_out, w_in, w_out)])
    mixed, grad_tokens, grad_w_in, grad_w_out, grad_router = pl.pallas_call(
        functools.partial(put_out, len(outs)),
        out_shape=outs,
        in_specs=[anywhere] * len(outs),
        out_specs=(hbm,) * len(outs),
        scratch_shapes=[pltpu.SemaphoreType.DMA((len(outs),))],
        compiler_params=pltpu.CompilerParams(vmem_limit_bytes=2**20),
        name="put_out",
    )(*results)
    return mixed, grad_tokens, grad_router, grad_w_in, grad_w_out


def solution(mesh):
    return jax.shard_map(
        functools.partial(on_device, mesh.shape["seq"], mesh.shape["exp"]),
        mesh=mesh,
        in_specs=(
            P(None, ("seq", "exp"), None),
            P(),
            P("exp", None, "seq"),
            P("exp", "seq", None),
            P(None, ("seq", "exp"), None),
        ),
        out_specs=(
            P(None, ("seq", "exp"), None),
            P(None, ("seq", "exp"), None),
            P(("seq", "exp"), None),
            P("exp", None, "seq"),
            P("exp", "seq", None),
        ),
        check_vma=False,
    )
```

```python
import functools

import jax
import jax.numpy as jnp
from jax import lax
from jax.experimental import pallas as pl
from jax.experimental.pallas import tpu as pltpu
from jax.sharding import PartitionSpec as P

MESH = pl.DeviceIdType.MESH
F32 = jnp.float32
BF16 = jnp.bfloat16
NT = (((1,), (1,)), ((), ()))
VMEM_BYTES = 67043328


def dot(a, b):
    return jnp.dot(a, b, preferred_element_type=F32)


def dot_nt(a, b):
    return lax.dot_general(a, b, NT, preferred_element_type=F32)


def place(seq_n, exp_n):
    s = lax.axis_index("seq")
    e = lax.axis_index("exp")
    half = exp_n // 2
    h, par = e // 2, e % 2
    pair = (s, h * 2 + (1 - par))
    seq_peers = [((s + k) % seq_n, e) for k in range(1, seq_n)]
    exp_peers = [(s, ((h + k) % half) * 2 + par) for k in range(1, half)]
    ways = [(a, b) for a in range(seq_n) for b in range(half) if a or b]
    there = [((s + a) % seq_n, (h + b) % half) for a, b in ways]
    return s, h, par, pair, seq_peers, exp_peers, ways, there


class Net:
    def __init__(self, send_sem, recv_sem):
        self.send_sem, self.recv_sem, self.groups = send_sem, recv_sem, []

    def group(self, whole):
        self.groups.append(whole)
        return Group(self, len(self.groups) - 1, whole)

    def drain(self):
        for i, whole in enumerate(self.groups):
            pltpu.make_async_copy(whole, whole, self.send_sem.at[i]).wait()


class Group:
    def __init__(self, net, index, whole):
        self.net, self.index, self.whole = net, index, whole

    def start(self, src, dst, peer):
        pltpu.make_async_remote_copy(
            src_ref=src,
            dst_ref=dst,
            send_sem=self.net.send_sem.at[self.index],
            recv_sem=self.net.recv_sem.at[self.index],
            device_id=peer,
            device_id_type=MESH,
        ).start()
        return self

    def show(self, peers, ref, *at):
        for peer in peers:
            self.start(ref.at[at], ref.at[at], peer)
        return self

    def arrived(self):
        pltpu.make_async_copy(self.whole, self.whole, self.net.recv_sem.at[self.index]).wait()


def groups_of(seq_n, exp_n):
    return 23 + (seq_n - 1) + 2 * (exp_n // 2 - 1)


def stat_tile(columns):
    shape = columns[0].shape[:-1] + (128,)
    lane = lax.broadcasted_iota(jnp.int32, shape, len(shape) - 1)
    tile = jnp.zeros(shape, F32)
    for i, column in enumerate(columns):
        tile = jnp.where(lane == i, column, tile)
    return tile


def by_clip(column, clips):
    owned = column.shape[-2] // clips
    return [column[..., c * owned : (c + 1) * owned, :] for c in range(clips)]


def split_stats(tile, clips):
    lanes = [tile[..., i : i + 1] for i in range(2 * clips)]
    axis = len(tile.shape) - 2
    return jnp.concatenate(lanes[:clips], axis=axis), jnp.concatenate(lanes[clips:], axis=axis)


def join(parts):
    peak = parts[0][0]
    for p, _ in parts[1:]:
        peak = jnp.maximum(peak, p)
    factors = [jnp.exp(p - peak) for p, _ in parts]
    mass = factors[0] * parts[0][1]
    for f, (_, m) in zip(factors[1:], parts[1:]):
        mass = mass + f * m
    return peak, mass, factors


def layer(
    seq_n, exp_n, tok_hbm, rt_hbm, gout_hbm, win_hbm, wout_hbm,
    mixed, gt, gwin, gwout, gr_o,
    tok, gout, rt, win, wout, tok_t, gout_t, win_t, wout_t, lg, qf, dsp, lm, xt, qt,
    buf_a, rcv_a, xb, xr, xg, gb, gbr, gc, gcr, gg, fe, fer, se, so_ag, sig_ag,
    st_a, st_p, st_b, st_z, st_c, sa, si,
    gr_a, gr_p, gr_b, gr_r,
    w_sem, send_sem, recv_sem,
):
    clips, rows, width = tok.shape
    slots = rt.shape[0]
    half = exp_n // 2
    owned = slots // exp_n
    nr = clips * owned
    dc = width // seq_n
    cuts = [slice(j * (width // 2), (j + 1) * (width // 2)) for j in range(2)]
    experts = win.shape[0]
    s, h, par, pair, seq_peers, exp_peers, ways, there = place(seq_n, exp_n)
    far_peers = [(t, g * 2 + par) for t, g in there]

    load_rt = pltpu.make_async_copy(rt_hbm, rt, w_sem.at[0])
    load_tok = [
        pltpu.make_async_copy(tok_hbm.at[c], tok.at[c], w_sem.at[3 + clips + c]) for c in range(clips)
    ]
    load_gout = [
        pltpu.make_async_copy(gout_hbm.at[c], gout.at[c], w_sem.at[1 + c]) for c in range(clips)
    ]
    load_in = pltpu.make_async_copy(win_hbm, win, w_sem.at[1 + clips])
    load_out = pltpu.make_async_copy(wout_hbm, wout, w_sem.at[2 + clips])
    load_rt.start()
    for load in load_tok + load_gout:
        load.start()
    barrier = pltpu.get_barrier_semaphore()
    for peer in [pair] + far_peers:
        pl.semaphore_signal(barrier, inc=1, device_id=peer, device_id_type=MESH)
    net = Net(send_sem, recv_sem)

    load_rt.wait()
    values, peaks, masses = [], [], []
    for c in range(clips):
        load_tok[c].wait()
        values.append(dot_nt(rt[...], tok[c]))
    for c, value in enumerate(values):
        lg[c] = value
        peak = jnp.max(value, axis=1, keepdims=True)
        p = jnp.exp(value - peak)
        peaks.append(peak.reshape(half, 2, owned, 1))
        masses.append(jnp.sum(p, axis=1, keepdims=True).reshape(half, 2, owned, 1))
        xt[c] = p.astype(BF16)
    for c, value in enumerate(values):
        q = jnp.exp(value - jnp.max(value, axis=0, keepdims=True))
        q = q / jnp.sum(q, axis=0, keepdims=True)
        qf[c] = q
        qt[c] = q.astype(BF16)
    tile = stat_tile(peaks + masses)
    for q in range(2):
        st_a[q] = tile[:, q]

    def lay_out(kind, values):
        for g in range(half):
            for q in range(2):
                at = (2 * g + q) * owned
                rows_ = [value[at : at + owned] for value in values]
                buf_a[kind, q, g] = jnp.concatenate(rows_, axis=0).astype(BF16)

    def pair_sum(kind, g, factors=None):
        mine = buf_a[kind, par, g].astype(F32)
        other = rcv_a[kind, g].astype(F32)
        if factors is not None:
            mine, other = mine * factors[0][g], other * factors[1][g]
        return (mine + other).astype(BF16)

    def spread_over(peers, at, ref, dst):
        group = net.group(dst)
        for k, peer in enumerate(peers):
            group.start(ref.at[at(k)], dst.at[k], peer)
        return group

    def show_seq(ref):
        return net.group(ref.at[pl.ds(0, seq_n - 1)]).show(seq_peers, ref, s)

    def exp_of(k):
        return (h + 1 + k) % half

    def seq_of(k):
        return (s + 1 + k) % seq_n

    def add_up(parts, factors=None):
        parts = [part.astype(F32) for part in parts]
        if factors is not None:
            parts = [part * f for part, f in zip(parts, factors)]
        total = parts[0]
        for part in parts[1:]:
            total = total + part
        return total

    lay_out(0, [dot(xt[c], tok[c]) for c in range(clips)])
    pl.semaphore_wait(barrier, 1 + len(far_peers))
    stat = net.group(st_p).start(st_a.at[1 - par], st_p, pair)
    inputs = net.group(rcv_a.at[0]).start(buf_a.at[0, 1 - par], rcv_a.at[0], pair)
    for load in load_gout:
        load.wait()
    lay_out(1, [dot(qt[c], gout[c]) for c in range(clips)])
    grads = net.group(rcv_a.at[1]).start(buf_a.at[1, 1 - par], rcv_a.at[1], pair)
    load_out.start()
    load_in.start()

    stat.arrived()
    peak, mass, fac = join([split_stats(st_a[par], clips), split_stats(st_p[...], clips)])
    st_b[...] = stat_tile(by_clip(peak, clips) + by_clip(mass, clips))
    stat = spread_over(exp_peers, exp_of, st_b, st_z)
    inputs.arrived()
    for g in range(half):
        xb[g] = pair_sum(0, g, fac)
    inputs = spread_over(exp_peers, exp_of, xb, xr)
    grads.arrived()
    for g in range(half):
        value = pair_sum(1, g)
        for t in range(seq_n):
            gb[t, g] = value[:, t * dc : (t + 1) * dc]
    grads = spread_over(seq_peers, seq_of, gb, gbr)
    for c in range(clips):
        tok_t[c] = tok[c].T
        gout_t[c] = gout[c].T
    stat.arrived()
    parts = [split_stats(st_b[h], clips)] + [split_stats(st_z[k], clips) for k in range(half - 1)]
    peak, mass, fac = join(parts)
    st_c[s] = stat_tile(by_clip(peak, clips) + by_clip(mass, clips))
    stat = show_seq(st_c)
    grads.arrived()
    for g in range(half):
        gc[g] = add_up([gb[s, g]] + [gbr[k, g] for k in range(seq_n - 1)]).astype(BF16)
    grads = spread_over(exp_peers, exp_of, gc, gcr)
    load_out.wait()
    load_in.wait()
    for e in range(experts // 2, experts):
        win_t[e] = win[e].T
    inputs.arrived()
    xg[s] = add_up([xb[h]] + [xr[k] for k in range(half - 1)], fac).astype(BF16)
    inputs = show_seq(xg)
    for e in range(experts):
        wout_t[e] = wout[e].T
    for e in range(experts // 2):
        win_t[e] = win[e].T
    stat.arrived()
    peak, mass, fac = join([split_stats(st_c[t], clips) for t in range(seq_n)])
    fac = [f / mass for f in fac]
    sa[h, par] = stat_tile(by_clip(peak, clips) + by_clip(mass, clips))
    stat_along = net.group(sa.at[pl.ds(0, half - 1), 0]).show(exp_peers, sa, h, par)
    stat_across = net.group(sa.at[pl.ds(0, half), 0]).show([pair], sa, h, par)
    grads.arrived()
    gg[s] = add_up([gc[h]] + [gcr[k] for k in range(half - 1)]).astype(BF16)
    grads = show_seq(gg)

    row = lax.broadcasted_iota(jnp.int32, (nr, 1), 0)
    expert_of = (row % owned) // (owned // experts)
    mask = [(expert_of == e).astype(F32) for e in range(experts)]
    inputs.arrived()
    x_rows = add_up([xg[t] for t in range(seq_n)], fac)
    pre = 0.0
    for e in range(experts):
        pre = pre + dot((x_rows * mask[e]).astype(BF16), win[e])
    hidden, back = jax.vjp(jax.nn.gelu, pre)
    out_part = 0.0
    for e in range(experts):
        out_part = out_part + dot((hidden * mask[e]).astype(BF16), wout[e])
    for t in range(seq_n):
        fe[t] = out_part[:, t * dc : (t + 1) * dc].astype(BF16)
    forward = spread_over(seq_peers, seq_of, fe, fer)
    grads.arrived()
    g_rows = jnp.concatenate([gg[t] for t in range(seq_n)], axis=1)
    hidden_grad = 0.0
    for e in range(experts):
        hidden_grad = hidden_grad + dot(g_rows, wout_t[e]) * mask[e]
    pre_grad = back(hidden_grad)[0]
    backward = []
    for j, cut in enumerate(cuts):
        in_part = 0.0
        for e in range(experts):
            in_part = in_part + dot((pre_grad * mask[e]).astype(BF16), win_t[e, :, cut])
        se[j, s] = in_part.astype(BF16)
        backward.append(net.group(se.at[j, pl.ds(0, seq_n - 1)]).show(seq_peers, se, j, s))

    def from_exp(k):
        return (h + half - 1 - k) % half

    def weight_grad(out, e, left, right):
        out[e] = dot((left * mask[e]).T.astype(BF16), right).astype(BF16)

    weight_grad(gwout, 0, hidden, g_rows)
    forward.arrived()
    so_ag[par, s, h] = add_up([fe[s]] + [fer[k] for k in range(seq_n - 1)]).astype(BF16)
    forward = []
    for a in range(seq_n):
        here = [peer for way, peer in zip(ways, far_peers) if way[0] == a]
        group = net.group(so_ag.at[0, 0, pl.ds(0, len(here))])
        group.show(here, so_ag, par, s, h)
        forward.append(group)
    columns = net.group(so_ag.at[0])
    stat_along.arrived()
    for k in range(half - 1):
        stat_across.show([pair], sa, from_exp(k), par)
    for e in range(1, experts):
        weight_grad(gwout, e, hidden, g_rows)
    pg = pre_grad.astype(BF16)
    inner, along, across = 0.0, [], []
    for j, cut in enumerate(cuts):
        backward[j].arrived()
        piece = add_up([se[j, t] for t in range(seq_n)]).astype(BF16)
        sig_ag[j, h, par] = piece
        inner = inner + jnp.sum(piece.astype(F32) * x_rows[:, cut], axis=1, keepdims=True)
        if j == len(cuts) - 1:
            si[h, par] = stat_tile(by_clip(inner, clips))
            inner_along = net.group(si.at[pl.ds(0, half - 1), 0]).show(exp_peers, si, h, par)
            inner_across = net.group(si.at[pl.ds(0, half), 0]).show([pair], si, h, par)
        along.append(
            [net.group(sig_ag.at[0, 0, 0]).show([peer], sig_ag, j, h, par) for peer in exp_peers]
        )
        across.append(net.group(sig_ag.at[0, pl.ds(0, half), 0]).show([pair], sig_ag, j, h, par))
    for e in range(experts):
        weight_grad(gwin, e, x_rows, pg)
    for a in range(seq_n):
        forward[a].arrived()
        columns.show([pair], so_ag, par, (s + seq_n - a) % seq_n)
    for j in range(len(cuts)):
        if j == len(cuts) - 1:
            inner_along.arrived()
            for k in range(half - 1):
                inner_across.show([pair], si, from_exp(k), par)
        for k in range(half - 1):
            along[j][k].arrived()
            across[j].show([pair], sig_ag, j, from_exp(k), par)

    def of_clip(value, c):
        return value.reshape(exp_n, clips, owned, value.shape[-1])[:, c].reshape(slots, value.shape[-1])

    def spread(value, c):
        value = value.reshape(exp_n, 1, owned, value.shape[-1])
        zero = jnp.zeros_like(value)
        parts = [value if k == c else zero for k in range(clips)]
        return jnp.concatenate(parts, axis=1).reshape(clips * slots, value.shape[-1])

    stat_across.arrived()
    columns.arrived()
    owners = [(g, q) for g in range(half) for q in range(2)]
    so = jnp.concatenate(
        [jnp.concatenate([so_ag[q, t, g] for t in range(seq_n)], axis=1) for g, q in owners], axis=0
    )
    stats = sa[...].reshape(slots, 128)
    for c in range(clips):
        mixing = qf[c]
        mixing_grad = of_clip(dot(so, gout_t[c]), c)
        lm[c] = mixing * (mixing_grad - jnp.sum(mixing * mixing_grad, axis=0, keepdims=True))
        mass = stats[:, clips + c : clips + c + 1]
        dsp[c] = jnp.exp(lg[c] - stats[:, c : c + 1]) / mass
    for j in range(len(cuts)):
        across[j].arrived()
    inner_across.arrived()
    sig = jnp.concatenate(
        [sig_ag[j].reshape(exp_n * nr, width // len(cuts)) for j in range(len(cuts))], axis=1
    )
    inners = si[...].reshape(slots, 128)
    gr = 0.0
    for c in range(clips):
        dispatch_grad = of_clip(dot(sig, tok_t[c]), c)
        lgrad = dsp[c] * (dispatch_grad - inners[:, c : c + 1]) + lm[c]
        lm[c] = lgrad
        gr = gr + dot(lgrad.astype(BF16), tok[c])

    out_rows = gr_o.shape[0]
    packed = gr_b.shape[2]
    pack = out_rows // packed
    whole = gr.T
    for t in range(seq_n):
        for g in range(half):
            for q in range(2):
                at = (t * exp_n + 2 * g + q) * out_rows
                parts = [whole[at + j * packed : at + (j + 1) * packed] for j in range(pack)]
                gr_a[q, t, g] = jnp.concatenate(parts, axis=1).astype(BF16)
    last = net.group(gr_p).start(gr_a.at[1 - par], gr_p, pair)
    both = jnp.concatenate([rt[...], sig], axis=0)

    def token_grad(c):
        left = jnp.concatenate([lm[c], spread(dsp[c], c)], axis=0)
        gt[c] = dot(left.T.astype(BF16), both).astype(BF16)

    last.arrived()
    gr_b[...] = (gr_a[par].astype(F32) + gr_p[...].astype(F32)).astype(BF16)
    last = net.group(gr_r)
    for k, (t, g) in enumerate(there):
        last.start(gr_b.at[t, g], gr_r.at[k], far_peers[k])
    for c in range(clips):
        mixed[c] = dot(spread(qf[c], c).T.astype(BF16), so).astype(BF16)
        token_grad(c)
    total = gr_b[s, h].astype(F32)
    last.arrived()
    for k in range(len(there)):
        total = total + gr_r[k].astype(F32)
    for j in range(pack):
        gr_o[j * packed : (j + 1) * packed] = total[:, j * slots : (j + 1) * slots]
    net.drain()
    assert len(net.groups) == groups_of(seq_n, exp_n)


def put_out(n, *refs):
    ins, outs, sem = refs[:n], refs[n : 2 * n], refs[2 * n]
    copies = []
    for src, dst in zip(ins, outs):
        copies.append(pltpu.make_async_copy(src, dst, sem.at[len(copies)]))
        copies[-1].start()
    for copy in copies:
        copy.wait()


def on_device(seq_n, exp_n, tokens, router, w_in, w_out, grad_out):
    clips, rows, width = tokens.shape
    slots = router.shape[1]
    experts, _, ff = w_in.shape
    half = exp_n // 2
    owned = slots // exp_n
    nr = clips * owned
    vmem = pl.BlockSpec(memory_space=pltpu.VMEM)
    hbm = pl.BlockSpec(memory_space=pltpu.HBM)
    anywhere = pl.BlockSpec(memory_space=pl.ANY)
    shape = jax.ShapeDtypeStruct
    out_rows = width // (seq_n * exp_n)
    pack = max(1, 128 // slots)
    tile = (out_rows // pack, slots * pack)
    piece = (nr, width)
    part = (nr, width // seq_n)
    stat = (owned, 128)
    n_groups = groups_of(seq_n, exp_n)
    outs = (
        shape(tokens.shape, BF16),
        shape(tokens.shape, BF16),
        shape(w_in.shape, BF16),
        shape(w_out.shape, BF16),
        shape((out_rows, slots), F32),
    )
    limit = VMEM_BYTES // 16 * 9
    results = pl.pallas_call(
        functools.partial(layer, seq_n, exp_n),
        out_shape=outs,
        in_specs=[hbm] * 5,
        out_specs=(vmem,) * 5,
        scratch_shapes=[
            pltpu.VMEM(tokens.shape, BF16),
            pltpu.VMEM(tokens.shape, BF16),
            pltpu.VMEM((slots, width), BF16),
            pltpu.VMEM(w_in.shape, BF16),
            pltpu.VMEM(w_out.shape, BF16),
            pltpu.VMEM((clips, width, rows), BF16),
            pltpu.VMEM((clips, width, rows), BF16),
            pltpu.VMEM((experts, ff, width), BF16),
            pltpu.VMEM((experts, width, ff), BF16),
            pltpu.VMEM((clips, slots, rows), F32),
            pltpu.VMEM((clips, slots, rows), F32),
            pltpu.VMEM((clips, slots, rows), F32),
            pltpu.VMEM((clips, slots, rows), F32),
            pltpu.VMEM((clips, slots, rows), BF16),
            pltpu.VMEM((clips, slots, rows), BF16),
            pltpu.VMEM((2, 2, half) + piece, BF16),
            pltpu.VMEM((2, half) + piece, BF16),
            pltpu.VMEM((half,) + piece, BF16),
            pltpu.VMEM((half - 1,) + piece, BF16),
            pltpu.VMEM((seq_n,) + piece, BF16),
            pltpu.VMEM((seq_n, half) + part, BF16),
            pltpu.VMEM((seq_n - 1, half) + part, BF16),
            pltpu.VMEM((half,) + part, BF16),
            pltpu.VMEM((half - 1,) + part, BF16),
            pltpu.VMEM((seq_n,) + part, BF16),
            pltpu.VMEM((seq_n,) + part, BF16),
            pltpu.VMEM((seq_n - 1,) + part, BF16),
            pltpu.VMEM((2, seq_n, nr, width // 2), BF16),
            pltpu.VMEM((2, seq_n, half) + part, BF16),
            pltpu.VMEM((2, half, 2, nr, width // 2), BF16),
            pltpu.VMEM((2, half) + stat, F32),
            pltpu.VMEM((half,) + stat, F32),
            pltpu.VMEM((half,) + stat, F32),
            pltpu.VMEM((half - 1,) + stat, F32),
            pltpu.VMEM((seq_n,) + stat, F32),
            pltpu.VMEM((half, 2) + stat, F32),
            pltpu.VMEM((half, 2) + stat, F32),
            pltpu.VMEM((2, seq_n, half) + tile, BF16),
            pltpu.VMEM((seq_n, half) + tile, BF16),
            pltpu.VMEM((seq_n, half) + tile, BF16),
            pltpu.VMEM((seq_n * half - 1,) + tile, BF16),
            pltpu.SemaphoreType.DMA((2 * clips + 3,)),
            pltpu.SemaphoreType.DMA((n_groups,)),
            pltpu.SemaphoreType.DMA((n_groups,)),
        ],
        compiler_params=pltpu.CompilerParams(
            collective_id=0, has_side_effects=True, vmem_limit_bytes=limit
        ),
        name="layer",
    )(*[pltpu.with_memory_space_constraint(a, pltpu.HBM) for a in (tokens, router.T, grad_out, w_in, w_out)])
    mixed, grad_tokens, grad_w_in, grad_w_out, grad_router = pl.pallas_call(
        functools.partial(put_out, len(outs)),
        out_shape=outs,
        in_specs=[anywhere] * len(outs),
        out_specs=(hbm,) * len(outs),
        scratch_shapes=[pltpu.SemaphoreType.DMA((len(outs),))],
        compiler_params=pltpu.CompilerParams(vmem_limit_bytes=2**20),
        name="put_out",
    )(*results)
    return mixed, grad_tokens, grad_router, grad_w_in, grad_w_out


def solution(mesh):
    return jax.shard_map(
        functools.partial(on_device, mesh.shape["seq"], mesh.shape["exp"]),
        mesh=mesh,
        in_specs=(
            P(None, ("seq", "exp"), None),
            P(),
            P("exp", None, "seq"),
            P("exp", "seq", None),
            P(None, ("seq", "exp"), None),
        ),
        out_specs=(
            P(None, ("seq", "exp"), None),
            P(None, ("seq", "exp"), None),
            P(("seq", "exp"), None),
            P("exp", None, "seq"),
            P("exp", "seq", None),
        ),
        check_vma=False,
    )
```

```python
import functools

import jax
import jax.numpy as jnp
from jax import lax
from jax.experimental import pallas as pl
from jax.experimental.pallas import tpu as pltpu
from jax.sharding import PartitionSpec as P

MESH = pl.DeviceIdType.MESH
F32 = jnp.float32
BF16 = jnp.bfloat16
NT = (((1,), (1,)), ((), ()))
VMEM_BYTES = 67043328


def dot(a, b):
    return jnp.dot(a, b, preferred_element_type=F32)


def dot_nt(a, b):
    return lax.dot_general(a, b, NT, preferred_element_type=F32)


def place(seq_n, exp_n):
    s = lax.axis_index("seq")
    e = lax.axis_index("exp")
    half = exp_n // 2
    h, par = e // 2, e % 2
    pair = (s, h * 2 + (1 - par))
    seq_peers = [((s + k) % seq_n, e) for k in range(1, seq_n)]
    exp_peers = [(s, ((h + k) % half) * 2 + par) for k in range(1, half)]
    ways = [(a, b) for a in range(seq_n) for b in range(half) if a or b]
    there = [((s + a) % seq_n, (h + b) % half) for a, b in ways]
    return s, h, par, pair, seq_peers, exp_peers, ways, there


class Net:
    def __init__(self, send_sem, recv_sem):
        self.send_sem, self.recv_sem, self.groups = send_sem, recv_sem, []

    def group(self, whole):
        self.groups.append(whole)
        return Group(self, len(self.groups) - 1, whole)

    def drain(self):
        for i, whole in enumerate(self.groups):
            pltpu.make_async_copy(whole, whole, self.send_sem.at[i]).wait()


class Group:
    def __init__(self, net, index, whole):
        self.net, self.index, self.whole = net, index, whole

    def start(self, src, dst, peer):
        pltpu.make_async_remote_copy(
            src_ref=src,
            dst_ref=dst,
            send_sem=self.net.send_sem.at[self.index],
            recv_sem=self.net.recv_sem.at[self.index],
            device_id=peer,
            device_id_type=MESH,
        ).start()
        return self

    def show(self, peers, ref, *at):
        for peer in peers:
            self.start(ref.at[at], ref.at[at], peer)
        return self

    def arrived(self):
        pltpu.make_async_copy(self.whole, self.whole, self.net.recv_sem.at[self.index]).wait()


def groups_of(seq_n, exp_n):
    return 23 + (seq_n - 1) + 2 * (exp_n // 2 - 1)


def stat_tile(columns):
    shape = columns[0].shape[:-1] + (128,)
    lane = lax.broadcasted_iota(jnp.int32, shape, len(shape) - 1)
    tile = jnp.zeros(shape, F32)
    for i, column in enumerate(columns):
        tile = jnp.where(lane == i, column, tile)
    return tile


def by_clip(column, clips):
    owned = column.shape[-2] // clips
    return [column[..., c * owned : (c + 1) * owned, :] for c in range(clips)]


def split_stats(tile, clips):
    lanes = [tile[..., i : i + 1] for i in range(2 * clips)]
    axis = len(tile.shape) - 2
    return jnp.concatenate(lanes[:clips], axis=axis), jnp.concatenate(lanes[clips:], axis=axis)


def join(parts):
    peak = parts[0][0]
    for p, _ in parts[1:]:
        peak = jnp.maximum(peak, p)
    factors = [jnp.exp(p - peak) for p, _ in parts]
    mass = factors[0] * parts[0][1]
    for f, (_, m) in zip(factors[1:], parts[1:]):
        mass = mass + f * m
    return peak, mass, factors


def layer(
    seq_n, exp_n, tok_hbm, rt_hbm, gout_hbm, win_hbm, wout_hbm,
    mixed, gt, gwin, gwout, gr_o,
    tok, gout, rt, win, wout, tok_t, gout_t, win_t, wout_t, lg, qf, dsp, lm, xt, qt,
    buf_a, rcv_a, xb, xr, xg, gb, gbr, gc, gcr, gg, fe, fer, se, so_ag, sig_ag,
    st_a, st_p, st_b, st_z, st_c, sa, si,
    gr_a, gr_p, gr_b, gr_r,
    w_sem, send_sem, recv_sem,
):
    clips, rows, width = tok.shape
    slots = rt.shape[0]
    half = exp_n // 2
    owned = slots // exp_n
    nr = clips * owned
    dc = width // seq_n
    cuts = [slice(j * (width // 2), (j + 1) * (width // 2)) for j in range(2)]
    experts = win.shape[0]
    s, h, par, pair, seq_peers, exp_peers, ways, there = place(seq_n, exp_n)
    far_peers = [(t, g * 2 + par) for t, g in there]

    load_rt = pltpu.make_async_copy(rt_hbm, rt, w_sem.at[0])
    load_tok = [
        pltpu.make_async_copy(tok_hbm.at[c], tok.at[c], w_sem.at[3 + clips + c]) for c in range(clips)
    ]
    load_gout = [
        pltpu.make_async_copy(gout_hbm.at[c], gout.at[c], w_sem.at[1 + c]) for c in range(clips)
    ]
    load_in = pltpu.make_async_copy(win_hbm, win, w_sem.at[1 + clips])
    load_out = pltpu.make_async_copy(wout_hbm, wout, w_sem.at[2 + clips])
    load_rt.start()
    for load in load_tok + load_gout:
        load.start()
    barrier = pltpu.get_barrier_semaphore()
    for peer in [pair] + far_peers:
        pl.semaphore_signal(barrier, inc=1, device_id=peer, device_id_type=MESH)
    net = Net(send_sem, recv_sem)

    load_rt.wait()
    values, peaks, masses = [], [], []
    for c in range(clips):
        load_tok[c].wait()
        values.append(dot_nt(rt[...], tok[c]))
    for c, value in enumerate(values):
        lg[c] = value
        peak = jnp.max(value, axis=1, keepdims=True)
        p = jnp.exp(value - peak)
        peaks.append(peak.reshape(half, 2, owned, 1))
        masses.append(jnp.sum(p, axis=1, keepdims=True).reshape(half, 2, owned, 1))
        xt[c] = p.astype(BF16)
    for c, value in enumerate(values):
        q = jnp.exp(value - jnp.max(value, axis=0, keepdims=True))
        q = q / jnp.sum(q, axis=0, keepdims=True)
        qf[c] = q
        qt[c] = q.astype(BF16)
    tile = stat_tile(peaks + masses)
    for q in range(2):
        st_a[q] = tile[:, q]

    def lay_out(kind, values):
        for g in range(half):
            for q in range(2):
                at = (2 * g + q) * owned
                rows_ = [value[at : at + owned] for value in values]
                buf_a[kind, q, g] = jnp.concatenate(rows_, axis=0).astype(BF16)

    def pair_sum(kind, g, factors=None):
        mine = buf_a[kind, par, g].astype(F32)
        other = rcv_a[kind, g].astype(F32)
        if factors is not None:
            mine, other = mine * factors[0][g], other * factors[1][g]
        return (mine + other).astype(BF16)

    def spread_over(peers, at, ref, dst):
        group = net.group(dst)
        for k, peer in enumerate(peers):
            group.start(ref.at[at(k)], dst.at[k], peer)
        return group

    def show_seq(ref):
        return net.group(ref.at[pl.ds(0, seq_n - 1)]).show(seq_peers, ref, s)

    def exp_of(k):
        return (h + 1 + k) % half

    def seq_of(k):
        return (s + 1 + k) % seq_n

    def add_up(parts, factors=None):
        parts = [part.astype(F32) for part in parts]
        if factors is not None:
            parts = [part * f for part, f in zip(parts, factors)]
        total = parts[0]
        for part in parts[1:]:
            total = total + part
        return total

    lay_out(0, [dot(xt[c], tok[c]) for c in range(clips)])
    pl.semaphore_wait(barrier, 1 + len(far_peers))
    stat = net.group(st_p).start(st_a.at[1 - par], st_p, pair)
    inputs = net.group(rcv_a.at[0]).start(buf_a.at[0, 1 - par], rcv_a.at[0], pair)
    for load in load_gout:
        load.wait()
    lay_out(1, [dot(qt[c], gout[c]) for c in range(clips)])
    grads = net.group(rcv_a.at[1]).start(buf_a.at[1, 1 - par], rcv_a.at[1], pair)
    load_out.start()
    load_in.start()

    stat.arrived()
    peak, mass, fac = join([split_stats(st_a[par], clips), split_stats(st_p[...], clips)])
    st_b[...] = stat_tile(by_clip(peak, clips) + by_clip(mass, clips))
    stat = spread_over(exp_peers, exp_of, st_b, st_z)
    inputs.arrived()
    for g in range(half):
        xb[g] = pair_sum(0, g, fac)
    inputs = spread_over(exp_peers, exp_of, xb, xr)
    grads.arrived()
    for g in range(half):
        value = pair_sum(1, g)
        for t in range(seq_n):
            gb[t, g] = value[:, t * dc : (t + 1) * dc]
    grads = spread_over(seq_peers, seq_of, gb, gbr)
    for c in range(clips):
        tok_t[c] = tok[c].T
        gout_t[c] = gout[c].T
    stat.arrived()
    parts = [split_stats(st_b[h], clips)] + [split_stats(st_z[k], clips) for k in range(half - 1)]
    peak, mass, fac = join(parts)
    st_c[s] = stat_tile(by_clip(peak, clips) + by_clip(mass, clips))
    stat = show_seq(st_c)
    grads.arrived()
    for g in range(half):
        gc[g] = add_up([gb[s, g]] + [gbr[k, g] for k in range(seq_n - 1)]).astype(BF16)
    grads = spread_over(exp_peers, exp_of, gc, gcr)
    load_out.wait()
    load_in.wait()
    for e in range(experts // 2, experts):
        win_t[e] = win[e].T
    inputs.arrived()
    xg[s] = add_up([xb[h]] + [xr[k] for k in range(half - 1)], fac).astype(BF16)
    inputs = show_seq(xg)
    for e in range(experts):
        wout_t[e] = wout[e].T
    for e in range(experts // 2):
        win_t[e] = win[e].T
    stat.arrived()
    peak, mass, fac = join([split_stats(st_c[t], clips) for t in range(seq_n)])
    fac = [f / mass for f in fac]
    sa[h, par] = stat_tile(by_clip(peak, clips) + by_clip(mass, clips))
    stat_along = net.group(sa.at[pl.ds(0, half - 1), 0]).show(exp_peers, sa, h, par)
    stat_across = net.group(sa.at[pl.ds(0, half), 0]).show([pair], sa, h, par)
    grads.arrived()
    gg[s] = add_up([gc[h]] + [gcr[k] for k in range(half - 1)]).astype(BF16)
    grads = show_seq(gg)

    row = lax.broadcasted_iota(jnp.int32, (nr, 1), 0)
    expert_of = (row % owned) // (owned // experts)
    mask = [(expert_of == e).astype(F32) for e in range(experts)]
    inputs.arrived()
    x_rows = add_up([xg[t] for t in range(seq_n)], fac)
    pre = 0.0
    for e in range(experts):
        pre = pre + dot((x_rows * mask[e]).astype(BF16), win[e])
    hidden, back = jax.vjp(jax.nn.gelu, pre)
    out_part = 0.0
    for e in range(experts):
        out_part = out_part + dot((hidden * mask[e]).astype(BF16), wout[e])
    for t in range(seq_n):
        fe[t] = out_part[:, t * dc : (t + 1) * dc].astype(BF16)
    forward = spread_over(seq_peers, seq_of, fe, fer)
    grads.arrived()
    g_rows = jnp.concatenate([gg[t] for t in range(seq_n)], axis=1)
    hidden_grad = 0.0
    for e in range(experts):
        hidden_grad = hidden_grad + dot(g_rows, wout_t[e]) * mask[e]
    pre_grad = back(hidden_grad)[0]
    backward = []
    for j, cut in enumerate(cuts):
        in_part = 0.0
        for e in range(experts):
            in_part = in_part + dot((pre_grad * mask[e]).astype(BF16), win_t[e, :, cut])
        se[s, :, cut] = in_part.astype(BF16)
        whole = net.group(se.at[pl.ds(0, seq_n - 1), :, cut])
        backward.append(whole.show(seq_peers, se, s, slice(None), cut))

    def from_exp(k):
        return (h + half - 1 - k) % half

    def weight_grad(out, e, left, right):
        out[e] = dot((left * mask[e]).T.astype(BF16), right).astype(BF16)

    weight_grad(gwout, 0, hidden, g_rows)
    forward.arrived()
    so_ag[par, s, h] = add_up([fe[s]] + [fer[k] for k in range(seq_n - 1)]).astype(BF16)
    forward = []
    for a in range(seq_n):
        here = [peer for way, peer in zip(ways, far_peers) if way[0] == a]
        group = net.group(so_ag.at[0, 0, pl.ds(0, len(here))])
        group.show(here, so_ag, par, s, h)
        forward.append(group)
    columns = net.group(so_ag.at[0])
    stat_along.arrived()
    for k in range(half - 1):
        stat_across.show([pair], sa, from_exp(k), par)
    for e in range(1, experts):
        weight_grad(gwout, e, hidden, g_rows)
    pg = pre_grad.astype(BF16)
    inner, along, across = 0.0, [], []
    for j, cut in enumerate(cuts):
        backward[j].arrived()
        piece = add_up([se[t, :, cut] for t in range(seq_n)]).astype(BF16)
        sig_ag[h, par, :, cut] = piece
        inner = inner + jnp.sum(piece.astype(F32) * x_rows[:, cut], axis=1, keepdims=True)
        if j == len(cuts) - 1:
            si[h, par] = stat_tile(by_clip(inner, clips))
            inner_along = net.group(si.at[pl.ds(0, half - 1), 0]).show(exp_peers, si, h, par)
            inner_across = net.group(si.at[pl.ds(0, half), 0]).show([pair], si, h, par)
        at = (h, par, slice(None), cut)
        along.append([net.group(sig_ag.at[0, 0, :, cut]).show([peer], sig_ag, *at) for peer in exp_peers])
        across.append(net.group(sig_ag.at[pl.ds(0, half), 0, :, cut]).show([pair], sig_ag, *at))
    for e in range(experts):
        weight_grad(gwin, e, x_rows, pg)
    for a in range(seq_n):
        forward[a].arrived()
        columns.show([pair], so_ag, par, (s + seq_n - a) % seq_n)
    for j, cut in enumerate(cuts):
        if j == len(cuts) - 1:
            inner_along.arrived()
            for k in range(half - 1):
                inner_across.show([pair], si, from_exp(k), par)
        for k in range(half - 1):
            along[j][k].arrived()
            across[j].show([pair], sig_ag, from_exp(k), par, slice(None), cut)

    def of_clip(value, c):
        return value.reshape(exp_n, clips, owned, value.shape[-1])[:, c].reshape(slots, value.shape[-1])

    def spread(value, c):
        value = value.reshape(exp_n, 1, owned, value.shape[-1])
        zero = jnp.zeros_like(value)
        parts = [value if k == c else zero for k in range(clips)]
        return jnp.concatenate(parts, axis=1).reshape(clips * slots, value.shape[-1])

    stat_across.arrived()
    stats = sa[...].reshape(slots, 128)
    for c in range(clips):
        mass = stats[:, clips + c : clips + c + 1]
        dsp[c] = jnp.exp(lg[c] - stats[:, c : c + 1]) / mass
    columns.arrived()
    owners = [(g, q) for g in range(half) for q in range(2)]
    so = jnp.concatenate(
        [jnp.concatenate([so_ag[q, t, g] for t in range(seq_n)], axis=1) for g, q in owners], axis=0
    )
    for c in range(clips):
        mixing = qf[c]
        mixing_grad = of_clip(dot(so, gout_t[c]), c)
        lm[c] = mixing * (mixing_grad - jnp.sum(mixing * mixing_grad, axis=0, keepdims=True))
    for j in range(len(cuts)):
        across[j].arrived()
    inner_across.arrived()
    sig = sig_ag[...].reshape(exp_n * nr, width)
    inners = si[...].reshape(slots, 128)
    gr = 0.0
    for c in range(clips):
        dispatch_grad = of_clip(dot(sig, tok_t[c]), c)
        lgrad = dsp[c] * (dispatch_grad - inners[:, c : c + 1]) + lm[c]
        lm[c] = lgrad
        gr = gr + dot(lgrad.astype(BF16), tok[c])

    out_rows = gr_o.shape[0]
    packed = gr_b.shape[2]
    pack = out_rows // packed
    whole = gr.T
    for t in range(seq_n):
        for g in range(half):
            for q in range(2):
                at = (t * exp_n + 2 * g + q) * out_rows
                parts = [whole[at + j * packed : at + (j + 1) * packed] for j in range(pack)]
                gr_a[q, t, g] = jnp.concatenate(parts, axis=1).astype(BF16)
    last = net.group(gr_p).start(gr_a.at[1 - par], gr_p, pair)
    both = jnp.concatenate([rt[...], sig], axis=0)

    def token_grad(c):
        left = jnp.concatenate([lm[c], spread(dsp[c], c)], axis=0)
        gt[c] = dot(left.T.astype(BF16), both).astype(BF16)

    last.arrived()
    gr_b[...] = (gr_a[par].astype(F32) + gr_p[...].astype(F32)).astype(BF16)
    last = net.group(gr_r)
    for k, (t, g) in enumerate(there):
        last.start(gr_b.at[t, g], gr_r.at[k], far_peers[k])
    for c in range(clips):
        mixed[c] = dot(spread(qf[c], c).T.astype(BF16), so).astype(BF16)
        token_grad(c)
    total = gr_b[s, h].astype(F32)
    last.arrived()
    for k in range(len(there)):
        total = total + gr_r[k].astype(F32)
    for j in range(pack):
        gr_o[j * packed : (j + 1) * packed] = total[:, j * slots : (j + 1) * slots]
    net.drain()
    assert len(net.groups) == groups_of(seq_n, exp_n)


def put_out(n, *refs):
    ins, outs, sem = refs[:n], refs[n : 2 * n], refs[2 * n]
    copies = []
    for src, dst in zip(ins, outs):
        copies.append(pltpu.make_async_copy(src, dst, sem.at[len(copies)]))
        copies[-1].start()
    for copy in copies:
        copy.wait()


def on_device(seq_n, exp_n, tokens, router, w_in, w_out, grad_out):
    clips, rows, width = tokens.shape
    slots = router.shape[1]
    experts, _, ff = w_in.shape
    half = exp_n // 2
    owned = slots // exp_n
    nr = clips * owned
    vmem = pl.BlockSpec(memory_space=pltpu.VMEM)
    hbm = pl.BlockSpec(memory_space=pltpu.HBM)
    anywhere = pl.BlockSpec(memory_space=pl.ANY)
    shape = jax.ShapeDtypeStruct
    out_rows = width // (seq_n * exp_n)
    pack = max(1, 128 // slots)
    tile = (out_rows // pack, slots * pack)
    piece = (nr, width)
    part = (nr, width // seq_n)
    stat = (owned, 128)
    n_groups = groups_of(seq_n, exp_n)
    outs = (
        shape(tokens.shape, BF16),
        shape(tokens.shape, BF16),
        shape(w_in.shape, BF16),
        shape(w_out.shape, BF16),
        shape((out_rows, slots), F32),
    )
    limit = VMEM_BYTES // 16 * 9
    results = pl.pallas_call(
        functools.partial(layer, seq_n, exp_n),
        out_shape=outs,
        in_specs=[hbm] * 5,
        out_specs=(vmem,) * 5,
        scratch_shapes=[
            pltpu.VMEM(tokens.shape, BF16),
            pltpu.VMEM(tokens.shape, BF16),
            pltpu.VMEM((slots, width), BF16),
            pltpu.VMEM(w_in.shape, BF16),
            pltpu.VMEM(w_out.shape, BF16),
            pltpu.VMEM((clips, width, rows), BF16),
            pltpu.VMEM((clips, width, rows), BF16),
            pltpu.VMEM((experts, ff, width), BF16),
            pltpu.VMEM((experts, width, ff), BF16),
            pltpu.VMEM((clips, slots, rows), F32),
            pltpu.VMEM((clips, slots, rows), F32),
            pltpu.VMEM((clips, slots, rows), F32),
            pltpu.VMEM((clips, slots, rows), F32),
            pltpu.VMEM((clips, slots, rows), BF16),
            pltpu.VMEM((clips, slots, rows), BF16),
            pltpu.VMEM((2, 2, half) + piece, BF16),
            pltpu.VMEM((2, half) + piece, BF16),
            pltpu.VMEM((half,) + piece, BF16),
            pltpu.VMEM((half - 1,) + piece, BF16),
            pltpu.VMEM((seq_n,) + piece, BF16),
            pltpu.VMEM((seq_n, half) + part, BF16),
            pltpu.VMEM((seq_n - 1, half) + part, BF16),
            pltpu.VMEM((half,) + part, BF16),
            pltpu.VMEM((half - 1,) + part, BF16),
            pltpu.VMEM((seq_n,) + part, BF16),
            pltpu.VMEM((seq_n,) + part, BF16),
            pltpu.VMEM((seq_n - 1,) + part, BF16),
            pltpu.VMEM((seq_n,) + piece, BF16),
            pltpu.VMEM((2, seq_n, half) + part, BF16),
            pltpu.VMEM((half, 2) + piece, BF16),
            pltpu.VMEM((2, half) + stat, F32),
            pltpu.VMEM((half,) + stat, F32),
            pltpu.VMEM((half,) + stat, F32),
            pltpu.VMEM((half - 1,) + stat, F32),
            pltpu.VMEM((seq_n,) + stat, F32),
            pltpu.VMEM((half, 2) + stat, F32),
            pltpu.VMEM((half, 2) + stat, F32),
            pltpu.VMEM((2, seq_n, half) + tile, BF16),
            pltpu.VMEM((seq_n, half) + tile, BF16),
            pltpu.VMEM((seq_n, half) + tile, BF16),
            pltpu.VMEM((seq_n * half - 1,) + tile, BF16),
            pltpu.SemaphoreType.DMA((2 * clips + 3,)),
            pltpu.SemaphoreType.DMA((n_groups,)),
            pltpu.SemaphoreType.DMA((n_groups,)),
        ],
        compiler_params=pltpu.CompilerParams(
            collective_id=0, has_side_effects=True, vmem_limit_bytes=limit
        ),
        name="layer",
    )(*[pltpu.with_memory_space_constraint(a, pltpu.HBM) for a in (tokens, router.T, grad_out, w_in, w_out)])
    mixed, grad_tokens, grad_w_in, grad_w_out, grad_router = pl.pallas_call(
        functools.partial(put_out, len(outs)),
        out_shape=outs,
        in_specs=[anywhere] * len(outs),
        out_specs=(hbm,) * len(outs),
        scratch_shapes=[pltpu.SemaphoreType.DMA((len(outs),))],
        compiler_params=pltpu.CompilerParams(vmem_limit_bytes=2**20),
        name="put_out",
    )(*results)
    return mixed, grad_tokens, grad_router, grad_w_in, grad_w_out


def solution(mesh):
    return jax.shard_map(
        functools.partial(on_device, mesh.shape["seq"], mesh.shape["exp"]),
        mesh=mesh,
        in_specs=(
            P(None, ("seq", "exp"), None),
            P(),
            P("exp", None, "seq"),
            P("exp", "seq", None),
            P(None, ("seq", "exp"), None),
        ),
        out_specs=(
            P(None, ("seq", "exp"), None),
            P(None, ("seq", "exp"), None),
            P(("seq", "exp"), None),
            P("exp", None, "seq"),
            P("exp", "seq", None),
        ),
        check_vma=False,
    )
```

```python
import functools

import jax
import jax.numpy as jnp
from jax import lax
from jax.experimental import pallas as pl
from jax.experimental.pallas import tpu as pltpu
from jax.sharding import PartitionSpec as P

MESH = pl.DeviceIdType.MESH
F32 = jnp.float32
BF16 = jnp.bfloat16
NT = (((1,), (1,)), ((), ()))
VMEM_BYTES = 67043328
SENDS = 16


def dot(a, b):
    return jnp.dot(a, b, preferred_element_type=F32)


def dot_nt(a, b):
    return lax.dot_general(a, b, NT, preferred_element_type=F32)


def place(seq_n, exp_n):
    s = lax.axis_index("seq")
    e = lax.axis_index("exp")
    half = exp_n // 2
    h, par = e // 2, e % 2
    pair = (s, h * 2 + (1 - par))
    seq_peers = [((s + k) % seq_n, e) for k in range(1, seq_n)]
    exp_peers = [(s, ((h + k) % half) * 2 + par) for k in range(1, half)]
    ways = [(a, b) for a in range(seq_n) for b in range(half) if a or b]
    there = [((s + a) % seq_n, (h + b) % half) for a, b in ways]
    return s, h, par, pair, seq_peers, exp_peers, ways, there


class Net:
    def __init__(self, send_sem, recv_sem):
        self.send_sem, self.recv_sem, self.groups = send_sem, recv_sem, []

    def group(self, whole):
        if len(self.groups) >= SENDS:
            self.sent(len(self.groups) - SENDS)
        self.groups.append(whole)
        return Group(self, len(self.groups) - 1, whole)

    def drain(self):
        for i in range(max(0, len(self.groups) - SENDS), len(self.groups)):
            self.sent(i)

    def sent(self, i):
        whole = self.groups[i]
        pltpu.make_async_copy(whole, whole, self.send_sem.at[i % SENDS]).wait()


class Group:
    def __init__(self, net, index, whole):
        self.net, self.index, self.whole = net, index, whole

    def start(self, src, dst, peer):
        pltpu.make_async_remote_copy(
            src_ref=src,
            dst_ref=dst,
            send_sem=self.net.send_sem.at[self.index % SENDS],
            recv_sem=self.net.recv_sem.at[self.index],
            device_id=peer,
            device_id_type=MESH,
        ).start()
        return self

    def show(self, peers, ref, *at):
        for peer in peers:
            self.start(ref.at[at], ref.at[at], peer)
        return self

    def arrived(self):
        pltpu.make_async_copy(self.whole, self.whole, self.net.recv_sem.at[self.index]).wait()


def groups_of(seq_n, exp_n):
    return 23 + (seq_n - 1) + 2 * (exp_n // 2 - 1)


def stat_tile(columns):
    shape = columns[0].shape[:-1] + (128,)
    lane = lax.broadcasted_iota(jnp.int32, shape, len(shape) - 1)
    tile = jnp.zeros(shape, F32)
    for i, column in enumerate(columns):
        tile = jnp.where(lane == i, column, tile)
    return tile


def by_clip(column, clips):
    owned = column.shape[-2] // clips
    return [column[..., c * owned : (c + 1) * owned, :] for c in range(clips)]


def split_stats(tile, clips):
    lanes = [tile[..., i : i + 1] for i in range(2 * clips)]
    axis = len(tile.shape) - 2
    return jnp.concatenate(lanes[:clips], axis=axis), jnp.concatenate(lanes[clips:], axis=axis)


def join(parts):
    peak = parts[0][0]
    for p, _ in parts[1:]:
        peak = jnp.maximum(peak, p)
    factors = [jnp.exp(p - peak) for p, _ in parts]
    mass = factors[0] * parts[0][1]
    for f, (_, m) in zip(factors[1:], parts[1:]):
        mass = mass + f * m
    return peak, mass, factors


def layer(
    seq_n, exp_n, tok_hbm, rt_hbm, gout_hbm, win_hbm, wout_hbm,
    mixed, gt, gwin, gwout, gr_o,
    tok, gout, rt, win, wout, tok_t, gout_t, win_t, wout_t, lg, qf, dsp, lm, xt, qt,
    buf_a, rcv_a, xb, xr, xg, gb, gbr, gc, gcr, gg, fe, fer, se, so_ag, sig_ag,
    st_a, st_p, st_b, st_z, st_c, sa, si,
    gr_a, gr_p, gr_b, gr_r,
    w_sem, send_sem, recv_sem,
):
    clips, rows, width = tok.shape
    slots = rt.shape[0]
    half = exp_n // 2
    owned = slots // exp_n
    nr = clips * owned
    dc = width // seq_n
    cuts = [slice(j * (width // 2), (j + 1) * (width // 2)) for j in range(2)]
    experts = win.shape[0]
    s, h, par, pair, seq_peers, exp_peers, ways, there = place(seq_n, exp_n)
    far_peers = [(t, g * 2 + par) for t, g in there]

    load_rt = pltpu.make_async_copy(rt_hbm, rt, w_sem.at[0])
    first = rows // 384 * 128
    spans = [(0, pl.ds(0, first)), (0, pl.ds(first, rows - first))]
    spans += [(c, pl.ds(0, rows)) for c in range(1, clips)]
    load_tok = [
        pltpu.make_async_copy(tok_hbm.at[at], tok.at[at], w_sem.at[2 + clips + i + 1])
        for i, at in enumerate(spans)
    ]
    load_gout = [
        pltpu.make_async_copy(gout_hbm.at[c], gout.at[c], w_sem.at[1 + c]) for c in range(clips)
    ]
    load_in = pltpu.make_async_copy(win_hbm, win, w_sem.at[1 + clips])
    load_out = pltpu.make_async_copy(wout_hbm, wout, w_sem.at[2 + clips])
    load_rt.start()
    for load in load_tok + load_gout:
        load.start()
    barrier = pltpu.get_barrier_semaphore()
    for peer in [pair] + far_peers:
        pl.semaphore_signal(barrier, inc=1, device_id=peer, device_id_type=MESH)
    net = Net(send_sem, recv_sem)

    load_rt.wait()
    values, peaks, masses = [], [], []
    for load, at in zip(load_tok, spans):
        load.wait()
        values.append(dot_nt(rt[...], tok[at]))
    values = [jnp.concatenate(values[:2], axis=1)] + values[2:]
    for c, value in enumerate(values):
        lg[c] = value
        peak = jnp.max(value, axis=1, keepdims=True)
        p = jnp.exp(value - peak)
        peaks.append(peak.reshape(half, 2, owned, 1))
        masses.append(jnp.sum(p, axis=1, keepdims=True).reshape(half, 2, owned, 1))
        xt[c] = p.astype(BF16)
    for c, value in enumerate(values):
        q = jnp.exp(value - jnp.max(value, axis=0, keepdims=True))
        q = q / jnp.sum(q, axis=0, keepdims=True)
        qf[c] = q
        qt[c] = q.astype(BF16)
    tile = stat_tile(peaks + masses)
    for q in range(2):
        st_a[q] = tile[:, q]

    def lay_out(kind, values):
        for g in range(half):
            for q in range(2):
                at = (2 * g + q) * owned
                rows_ = [value[at : at + owned] for value in values]
                buf_a[kind, q, g] = jnp.concatenate(rows_, axis=0).astype(BF16)

    def pair_sum(kind, g, factors=None):
        mine = buf_a[kind, par, g].astype(F32)
        other = rcv_a[kind, g].astype(F32)
        if factors is not None:
            mine, other = mine * factors[0][g], other * factors[1][g]
        return (mine + other).astype(BF16)

    def spread_over(peers, at, ref, dst):
        group = net.group(dst)
        for k, peer in enumerate(peers):
            group.start(ref.at[at(k)], dst.at[k], peer)
        return group

    def show_seq(ref):
        return net.group(ref.at[pl.ds(0, seq_n - 1)]).show(seq_peers, ref, s)

    def exp_of(k):
        return (h + 1 + k) % half

    def seq_of(k):
        return (s + 1 + k) % seq_n

    def add_up(parts, factors=None):
        parts = [part.astype(F32) for part in parts]
        if factors is not None:
            parts = [part * f for part, f in zip(parts, factors)]
        total = parts[0]
        for part in parts[1:]:
            total = total + part
        return total

    lay_out(0, [dot(xt[c], tok[c]) for c in range(clips)])
    pl.semaphore_wait(barrier, 1 + len(far_peers))
    stat = net.group(st_p).start(st_a.at[1 - par], st_p, pair)
    inputs = net.group(rcv_a.at[0]).start(buf_a.at[0, 1 - par], rcv_a.at[0], pair)
    for load in load_gout:
        load.wait()
    lay_out(1, [dot(qt[c], gout[c]) for c in range(clips)])
    grads = net.group(rcv_a.at[1]).start(buf_a.at[1, 1 - par], rcv_a.at[1], pair)
    load_out.start()
    load_in.start()

    stat.arrived()
    peak, mass, fac = join([split_stats(st_a[par], clips), split_stats(st_p[...], clips)])
    st_b[...] = stat_tile(by_clip(peak, clips) + by_clip(mass, clips))
    stat = spread_over(exp_peers, exp_of, st_b, st_z)
    inputs.arrived()
    for g in range(half):
        xb[g] = pair_sum(0, g, fac)
    inputs = spread_over(exp_peers, exp_of, xb, xr)
    grads.arrived()
    for g in range(half):
        value = pair_sum(1, g)
        for t in range(seq_n):
            gb[t, g] = value[:, t * dc : (t + 1) * dc]
    grads = spread_over(seq_peers, seq_of, gb, gbr)
    for c in range(clips):
        tok_t[c] = tok[c].T
        gout_t[c] = gout[c].T
    stat.arrived()
    parts = [split_stats(st_b[h], clips)] + [split_stats(st_z[k], clips) for k in range(half - 1)]
    peak, mass, fac = join(parts)
    st_c[s] = stat_tile(by_clip(peak, clips) + by_clip(mass, clips))
    stat = show_seq(st_c)
    grads.arrived()
    for g in range(half):
        gc[g] = add_up([gb[s, g]] + [gbr[k, g] for k in range(seq_n - 1)]).astype(BF16)
    grads = spread_over(exp_peers, exp_of, gc, gcr)
    load_out.wait()
    load_in.wait()
    for e in range(experts // 2, experts):
        win_t[e] = win[e].T
    inputs.arrived()
    xg[s] = add_up([xb[h]] + [xr[k] for k in range(half - 1)], fac).astype(BF16)
    inputs = show_seq(xg)
    for e in range(experts):
        wout_t[e] = wout[e].T
    for e in range(experts // 2):
        win_t[e] = win[e].T
    stat.arrived()
    peak, mass, fac = join([split_stats(st_c[t], clips) for t in range(seq_n)])
    fac = [f / mass for f in fac]
    sa[h, par] = stat_tile(by_clip(peak, clips) + by_clip(mass, clips))
    stat_along = net.group(sa.at[pl.ds(0, half - 1), 0]).show(exp_peers, sa, h, par)
    stat_across = net.group(sa.at[pl.ds(0, half), 0]).show([pair], sa, h, par)
    grads.arrived()
    gg[s] = add_up([gc[h]] + [gcr[k] for k in range(half - 1)]).astype(BF16)
    grads = show_seq(gg)

    row = lax.broadcasted_iota(jnp.int32, (nr, 1), 0)
    expert_of = (row % owned) // (owned // experts)
    mask = [(expert_of == e).astype(F32) for e in range(experts)]
    inputs.arrived()
    x_rows = add_up([xg[t] for t in range(seq_n)], fac)
    pre = 0.0
    for e in range(experts):
        pre = pre + dot((x_rows * mask[e]).astype(BF16), win[e])
    hidden, back = jax.vjp(jax.nn.gelu, pre)
    out_part = 0.0
    for e in range(experts):
        out_part = out_part + dot((hidden * mask[e]).astype(BF16), wout[e])
    for t in range(seq_n):
        fe[t] = out_part[:, t * dc : (t + 1) * dc].astype(BF16)
    forward = spread_over(seq_peers, seq_of, fe, fer)
    grads.arrived()
    g_rows = jnp.concatenate([gg[t] for t in range(seq_n)], axis=1)
    hidden_grad = 0.0
    for e in range(experts):
        hidden_grad = hidden_grad + dot(g_rows, wout_t[e]) * mask[e]
    pre_grad = back(hidden_grad)[0]
    backward = []
    for j, cut in enumerate(cuts):
        in_part = 0.0
        for e in range(experts):
            in_part = in_part + dot((pre_grad * mask[e]).astype(BF16), win_t[e, :, cut])
        se[s, :, cut] = in_part.astype(BF16)
        whole = net.group(se.at[pl.ds(0, seq_n - 1), :, cut])
        backward.append(whole.show(seq_peers, se, s, slice(None), cut))

    def from_exp(k):
        return (h + half - 1 - k) % half

    def weight_grad(out, e, left, right):
        out[e] = dot((left * mask[e]).T.astype(BF16), right).astype(BF16)

    weight_grad(gwout, 0, hidden, g_rows)
    forward.arrived()
    so_ag[par, s, h] = add_up([fe[s]] + [fer[k] for k in range(seq_n - 1)]).astype(BF16)
    forward = []
    for a in range(seq_n):
        here = [peer for way, peer in zip(ways, far_peers) if way[0] == a]
        group = net.group(so_ag.at[0, 0, pl.ds(0, len(here))])
        group.show(here, so_ag, par, s, h)
        forward.append(group)
    columns = net.group(so_ag.at[0])
    stat_along.arrived()
    for k in range(half - 1):
        stat_across.show([pair], sa, from_exp(k), par)
    for e in range(1, experts):
        weight_grad(gwout, e, hidden, g_rows)
    pg = pre_grad.astype(BF16)
    inner, along, across = 0.0, [], []
    for j, cut in enumerate(cuts):
        backward[j].arrived()
        piece = add_up([se[t, :, cut] for t in range(seq_n)]).astype(BF16)
        sig_ag[h, par, :, cut] = piece
        inner = inner + jnp.sum(piece.astype(F32) * x_rows[:, cut], axis=1, keepdims=True)
        if j == len(cuts) - 1:
            si[h, par] = stat_tile(by_clip(inner, clips))
            inner_along = net.group(si.at[pl.ds(0, half - 1), 0]).show(exp_peers, si, h, par)
            inner_across = net.group(si.at[pl.ds(0, half), 0]).show([pair], si, h, par)
        at = (h, par, slice(None), cut)
        along.append([net.group(sig_ag.at[0, 0, :, cut]).show([peer], sig_ag, *at) for peer in exp_peers])
        across.append(net.group(sig_ag.at[pl.ds(0, half), 0, :, cut]).show([pair], sig_ag, *at))
    for e in range(experts):
        weight_grad(gwin, e, x_rows, pg)
    for a in range(seq_n):
        forward[a].arrived()
        columns.show([pair], so_ag, par, (s + seq_n - a) % seq_n)
    for j, cut in enumerate(cuts):
        if j == len(cuts) - 1:
            inner_along.arrived()
            for k in range(half - 1):
                inner_across.show([pair], si, from_exp(k), par)
        for k in range(half - 1):
            along[j][k].arrived()
            across[j].show([pair], sig_ag, from_exp(k), par, slice(None), cut)

    def of_clip(value, c):
        return value.reshape(exp_n, clips, owned, value.shape[-1])[:, c].reshape(slots, value.shape[-1])

    def spread(value, c):
        value = value.reshape(exp_n, 1, owned, value.shape[-1])
        zero = jnp.zeros_like(value)
        parts = [value if k == c else zero for k in range(clips)]
        return jnp.concatenate(parts, axis=1).reshape(clips * slots, value.shape[-1])

    stat_across.arrived()
    stats = sa[...].reshape(slots, 128)
    for c in range(clips):
        mass = stats[:, clips + c : clips + c + 1]
        dsp[c] = jnp.exp(lg[c] - stats[:, c : c + 1]) / mass
    columns.arrived()
    owners = [(g, q) for g in range(half) for q in range(2)]
    so = jnp.concatenate(
        [jnp.concatenate([so_ag[q, t, g] for t in range(seq_n)], axis=1) for g, q in owners], axis=0
    )
    for c in range(clips):
        mixing = qf[c]
        mixing_grad = of_clip(dot(so, gout_t[c]), c)
        lm[c] = mixing * (mixing_grad - jnp.sum(mixing * mixing_grad, axis=0, keepdims=True))
    for j in range(len(cuts)):
        across[j].arrived()
    inner_across.arrived()
    sig = sig_ag[...].reshape(exp_n * nr, width)
    inners = si[...].reshape(slots, 128)
    gr = 0.0
    for c in range(clips):
        dispatch_grad = of_clip(dot(sig, tok_t[c]), c)
        lgrad = dsp[c] * (dispatch_grad - inners[:, c : c + 1]) + lm[c]
        lm[c] = lgrad
        gr = gr + dot(lgrad.astype(BF16), tok[c])

    out_rows = gr_o.shape[0]
    packed = gr_b.shape[2]
    pack = out_rows // packed
    whole = gr.T
    for t in range(seq_n):
        for g in range(half):
            for q in range(2):
                at = (t * exp_n + 2 * g + q) * out_rows
                parts = [whole[at + j * packed : at + (j + 1) * packed] for j in range(pack)]
                gr_a[q, t, g] = jnp.concatenate(parts, axis=1).astype(BF16)
    last = net.group(gr_p).start(gr_a.at[1 - par], gr_p, pair)
    both = jnp.concatenate([rt[...], sig], axis=0)

    def token_grad(c):
        left = jnp.concatenate([lm[c], spread(dsp[c], c)], axis=0)
        gt[c] = dot(left.T.astype(BF16), both).astype(BF16)

    last.arrived()
    gr_b[...] = (gr_a[par].astype(F32) + gr_p[...].astype(F32)).astype(BF16)
    last = net.group(gr_r)
    for k, (t, g) in enumerate(there):
        last.start(gr_b.at[t, g], gr_r.at[k], far_peers[k])
    for c in range(clips):
        mixed[c] = dot(spread(qf[c], c).T.astype(BF16), so).astype(BF16)
        token_grad(c)
    total = gr_b[s, h].astype(F32)
    last.arrived()
    for k in range(len(there)):
        total = total + gr_r[k].astype(F32)
    for j in range(pack):
        gr_o[j * packed : (j + 1) * packed] = total[:, j * slots : (j + 1) * slots]
    net.drain()
    assert len(net.groups) == groups_of(seq_n, exp_n)


def put_out(n, *refs):
    ins, outs, sem = refs[:n], refs[n : 2 * n], refs[2 * n]
    copies = []
    for src, dst in zip(ins, outs):
        copies.append(pltpu.make_async_copy(src, dst, sem.at[len(copies)]))
        copies[-1].start()
    for copy in copies:
        copy.wait()


def on_device(seq_n, exp_n, tokens, router, w_in, w_out, grad_out):
    clips, rows, width = tokens.shape
    slots = router.shape[1]
    experts, _, ff = w_in.shape
    half = exp_n // 2
    owned = slots // exp_n
    nr = clips * owned
    vmem = pl.BlockSpec(memory_space=pltpu.VMEM)
    hbm = pl.BlockSpec(memory_space=pltpu.HBM)
    anywhere = pl.BlockSpec(memory_space=pl.ANY)
    shape = jax.ShapeDtypeStruct
    out_rows = width // (seq_n * exp_n)
    pack = max(1, 128 // slots)
    tile = (out_rows // pack, slots * pack)
    piece = (nr, width)
    part = (nr, width // seq_n)
    stat = (owned, 128)
    n_groups = groups_of(seq_n, exp_n)
    outs = (
        shape(tokens.shape, BF16),
        shape(tokens.shape, BF16),
        shape(w_in.shape, BF16),
        shape(w_out.shape, BF16),
        shape((out_rows, slots), F32),
    )
    limit = VMEM_BYTES // 16 * 9
    results = pl.pallas_call(
        functools.partial(layer, seq_n, exp_n),
        out_shape=outs,
        in_specs=[hbm] * 5,
        out_specs=(vmem,) * 5,
        scratch_shapes=[
            pltpu.VMEM(tokens.shape, BF16),
            pltpu.VMEM(tokens.shape, BF16),
            pltpu.VMEM((slots, width), BF16),
            pltpu.VMEM(w_in.shape, BF16),
            pltpu.VMEM(w_out.shape, BF16),
            pltpu.VMEM((clips, width, rows), BF16),
            pltpu.VMEM((clips, width, rows), BF16),
            pltpu.VMEM((experts, ff, width), BF16),
            pltpu.VMEM((experts, width, ff), BF16),
            pltpu.VMEM((clips, slots, rows), F32),
            pltpu.VMEM((clips, slots, rows), F32),
            pltpu.VMEM((clips, slots, rows), F32),
            pltpu.VMEM((clips, slots, rows), F32),
            pltpu.VMEM((clips, slots, rows), BF16),
            pltpu.VMEM((clips, slots, rows), BF16),
            pltpu.VMEM((2, 2, half) + piece, BF16),
            pltpu.VMEM((2, half) + piece, BF16),
            pltpu.VMEM((half,) + piece, BF16),
            pltpu.VMEM((half - 1,) + piece, BF16),
            pltpu.VMEM((seq_n,) + piece, BF16),
            pltpu.VMEM((seq_n, half) + part, BF16),
            pltpu.VMEM((seq_n - 1, half) + part, BF16),
            pltpu.VMEM((half,) + part, BF16),
            pltpu.VMEM((half - 1,) + part, BF16),
            pltpu.VMEM((seq_n,) + part, BF16),
            pltpu.VMEM((seq_n,) + part, BF16),
            pltpu.VMEM((seq_n - 1,) + part, BF16),
            pltpu.VMEM((seq_n,) + piece, BF16),
            pltpu.VMEM((2, seq_n, half) + part, BF16),
            pltpu.VMEM((half, 2) + piece, BF16),
            pltpu.VMEM((2, half) + stat, F32),
            pltpu.VMEM((half,) + stat, F32),
            pltpu.VMEM((half,) + stat, F32),
            pltpu.VMEM((half - 1,) + stat, F32),
            pltpu.VMEM((seq_n,) + stat, F32),
            pltpu.VMEM((half, 2) + stat, F32),
            pltpu.VMEM((half, 2) + stat, F32),
            pltpu.VMEM((2, seq_n, half) + tile, BF16),
            pltpu.VMEM((seq_n, half) + tile, BF16),
            pltpu.VMEM((seq_n, half) + tile, BF16),
            pltpu.VMEM((seq_n * half - 1,) + tile, BF16),
            pltpu.SemaphoreType.DMA((2 * clips + 4,)),
            pltpu.SemaphoreType.DMA((SENDS,)),
            pltpu.SemaphoreType.DMA((n_groups,)),
        ],
        compiler_params=pltpu.CompilerParams(
            collective_id=0, has_side_effects=True, vmem_limit_bytes=limit
        ),
        name="layer",
    )(*[pltpu.with_memory_space_constraint(a, pltpu.HBM) for a in (tokens, router.T, grad_out, w_in, w_out)])
    mixed, grad_tokens, grad_w_in, grad_w_out, grad_router = pl.pallas_call(
        functools.partial(put_out, len(outs)),
        out_shape=outs,
        in_specs=[anywhere] * len(outs),
        out_specs=(hbm,) * len(outs),
        scratch_shapes=[pltpu.SemaphoreType.DMA((len(outs),))],
        compiler_params=pltpu.CompilerParams(vmem_limit_bytes=2**20),
        name="put_out",
    )(*results)
    return mixed, grad_tokens, grad_router, grad_w_in, grad_w_out


def solution(mesh):
    return jax.shard_map(
        functools.partial(on_device, mesh.shape["seq"], mesh.shape["exp"]),
        mesh=mesh,
        in_specs=(
            P(None, ("seq", "exp"), None),
            P(),
            P("exp", None, "seq"),
            P("exp", "seq", None),
            P(None, ("seq", "exp"), None),
        ),
        out_specs=(
            P(None, ("seq", "exp"), None),
            P(None, ("seq", "exp"), None),
            P(("seq", "exp"), None),
            P("exp", None, "seq"),
            P("exp", "seq", None),
        ),
        check_vma=False,
    )
```
